32 devices in a mesh: gx: 8 (over y, x, core), gy: 4 (over z).
Axes of the slice: x: 2, y: 2, z: 4, core: 2. Of those that a mesh axis runs over, the one named last changes fastest.
Arguments:
- density: float32 [32, 256, 256], P(('gx', 'gy')), may hold values from -0.06 to 0.56, as said below
- coupling: float32 [32, 256, 256], P(('gx', 'gy')), may hold values from -0.04 to 0.04
- weights: float32 [32], P(('gx', 'gy')), may hold values from 0.25 to 2
- live_mask: int32 [32], P(('gx', 'gy')), may hold values 0 or 1
- dimer_pairs: int32 [32, 2], replicated, may hold values from 0 to 31, as said below
- dimer_slot: int32 [32], replicated, may hold values from 0 to 31, as said below
- frag_slot: int32 [32], replicated, may hold values from 0 to 31, as said below
Outputs:
- refined: float32 [32, 256, 256], P(('gx', 'gy'))
The draws below stay inside these ranges and needn't reach their ends.
Inputs may be any that keep to these rules, and one draw needn't show every extreme that they name: `dimer_slot`: each slot holds exactly one listed dimer. `frag_slot`: each fragment has its own slot; slot q lies on device q, devices numbered with gy fastest. `dimer_pairs`: the two fragments of a dimer differ. The dimers in slots k * 1 to (k + 1) - 1 (device k) name 2 fragments whose storage devices have pairwise different gx indices and pairwise different gy indices. `density`: each block is symmetric.
All inputs are finite; a program needn't handle non-finite values. No bound on the sum of `live_mask` on one device may be relied on, other than what follows from the above.
Results may differ from the reference program's by a relative error of at most 0.0003.
Values sent between devices are 32-bit elements; how exact they have to be, the bound alone decides.
A program may use at most 64 MiB of HBM per device.

```python
import math
import jax
import jax.numpy as jnp
from jax import lax

B = 256
FRAG_DEV = 1
ITERS = 3
SWEEPS = 1
DIM_DEV = 1
FRAGMENTS = 32
DIMERS = 32
N_GX = 8
N_GY = 4


def routing_plan(key):
    frag_key = jax.random.fold_in(key, 101)
    dimer_key = jax.random.fold_in(key, 202)
    row_key = jax.random.fold_in(key, 303)
    column_key = jax.random.fold_in(key, 404)
    local_key = jax.random.fold_in(key, 505)
    frag_slot = jax.random.permutation(frag_key, FRAGMENTS).astype(jnp.int32)
    dimer_slot = jax.random.permutation(dimer_key, DIMERS).astype(jnp.int32)
    devices_all = N_GX * N_GY
    refs = 2 * DIM_DEV
    row_keys = jax.random.split(row_key, devices_all)
    column_keys = jax.random.split(column_key, devices_all)
    pick_x = jax.vmap(lambda one_key: jax.random.permutation(one_key, N_GX)[:refs])(row_keys)
    pick_y = jax.vmap(lambda one_key: jax.random.permutation(one_key, N_GY)[:refs])(column_keys)
    local_part = jax.random.randint(local_key, (devices_all, refs), 0, FRAG_DEV)
    ref_slot = ((pick_x * N_GY + pick_y) * FRAG_DEV + local_part).astype(jnp.int32).reshape(DIMERS, 2)
    inverse = jnp.argsort(frag_slot).astype(jnp.int32)
    slot_frags = inverse[ref_slot]
    dimer_pairs = slot_frags[dimer_slot]
    return (dimer_pairs.astype(jnp.int32), dimer_slot, frag_slot)


def draw_dimer_pairs(key, part):
    return routing_plan(key)[0]


def draw_dimer_slot(key, part):
    return routing_plan(key)[1]


def draw_frag_slot(key, part):
    return routing_plan(key)[2]


def draw_density(key, part):
    noise_key = jax.random.fold_in(key, 606)
    raw = jnp.clip(jax.random.normal(noise_key, (FRAGMENTS, B, B), jnp.float32), -4.0, 4.0)
    symmetric = (raw + jnp.swapaxes(raw, 1, 2)) * (0.01 / 1.4142135)
    return symmetric + 0.5 * jnp.eye(B, dtype=jnp.float32)[None, :, :]


def draw_coupling(key, part):
    noise_key = jax.random.fold_in(key, 707)
    raw = jnp.clip(jax.random.normal(noise_key, (DIMERS, B, B), jnp.float32), -4.0, 4.0)
    return raw * 0.01


def place_ends(drawn, key, low, largest):
    index_at = [jax.random.randint(jax.random.fold_in(key, axis), (), 0, length) for axis, length in enumerate(drawn.shape)]
    main_axis = drawn.shape.index(max(drawn.shape))
    beside = index_at[:main_axis] + [(index_at[main_axis] + 1) % drawn.shape[main_axis]] + index_at[main_axis + 1:]
    return drawn.at[tuple(index_at)].set(low).at[tuple(beside)].set(largest)


def shard_levels(rng, extent, cuts, least, high):
    factor_of, own = 1.0, jax.random.fold_in(rng, 6)
    for position, parts in cuts:
        steps = jnp.exp(jax.random.uniform(jax.random.fold_in(own, position), (parts,), jnp.float32, least / len(cuts), high / len(cuts)))
        factor_of = factor_of * jnp.repeat(steps, extent[position] // parts).reshape([-1 if axis == position else 1 for axis in range(len(extent))])
    return factor_of


def setup_inputs(seed: int = 0) -> dict:
    splits = jax.random.split(jax.random.key(seed), 8)
    density = draw_density(jax.random.fold_in(splits[7], 71), 0)
    coupling = draw_coupling(jax.random.fold_in(splits[7], 71), 0)
    weights = jnp.clip(jnp.exp(math.log(2.0) - 2.0794415 * jax.random.uniform(splits[2], (DIMERS,), jnp.float32) ** shard_levels(splits[2], (DIMERS,), ((0, 32),), -0.2, 0.2)), 0.25, 2.0)
    live_mask = place_ends((jax.random.randint(splits[3], (DIMERS,), 0, 4) < 3).astype(jnp.int32), jax.random.fold_in(splits[3], 1), 0, 1)
    dimer_pairs = draw_dimer_pairs(jax.random.fold_in(splits[7], 71), 0)
    dimer_slot = draw_dimer_slot(jax.random.fold_in(splits[7], 71), 0)
    frag_slot = draw_frag_slot(jax.random.fold_in(splits[7], 71), 0)
    return dict(density=density, coupling=coupling, weights=weights, live_mask=live_mask, dimer_pairs=dimer_pairs, dimer_slot=dimer_slot, frag_slot=frag_slot)


def product(left, right):
    return jnp.dot(left, right, precision=lax.Precision.HIGHEST, preferred_element_type=jnp.float32)


def purify(first_block, second_block, coupling_block):
    half_width = first_block.shape[0]
    upper_rows = jnp.concatenate([first_block, coupling_block], axis=1)
    lower_rows = jnp.concatenate([coupling_block.T, second_block], axis=1)
    matrix = jnp.concatenate([upper_rows, lower_rows], axis=0)
    for repeat in range(ITERS):
        square = product(matrix, matrix)
        matrix = 3.0 * square - 2.0 * product(square, matrix)
    return matrix[:half_width, :half_width], matrix[half_width:, half_width:]


def reference(density, coupling, weights, live_mask, dimer_pairs, dimer_slot, frag_slot):
    blocks = density
    for sweep_index in range(SWEEPS):
        def visit(carry, dimer_index):
            totals, weight_sums = carry
            slot_index = dimer_slot[dimer_index]
            first_slot = frag_slot[dimer_pairs[dimer_index, 0]]
            second_slot = frag_slot[dimer_pairs[dimer_index, 1]]
            factor = jnp.where(live_mask[slot_index] > 0, weights[slot_index], jnp.float32(0.0))
            first_new, second_new = purify(blocks[first_slot], blocks[second_slot], coupling[slot_index])
            totals = totals.at[first_slot].add(factor * first_new)
            totals = totals.at[second_slot].add(factor * second_new)
            weight_sums = weight_sums.at[first_slot].add(factor)
            weight_sums = weight_sums.at[second_slot].add(factor)
            return (totals, weight_sums), dimer_index

        start = (jnp.zeros(blocks.shape, jnp.float32), jnp.zeros((blocks.shape[0],), jnp.float32))
        finals, ignored = lax.scan(visit, start, jnp.arange(dimer_pairs.shape[0], dtype=jnp.int32))
        totals, weight_sums = finals
        blocks = (blocks + totals) / (1.0 + weight_sums)[:, None, None]
    return blocks
```

```python
import functools
import jax
import jax.numpy as jnp
from jax import lax
from jax.experimental import pallas as pl
from jax.experimental.pallas import tpu as pltpu
from jax.sharding import PartitionSpec as P

ITERS = 3
MESH = pl.DeviceIdType.MESH
F32 = jnp.float32
BF16 = jnp.bfloat16


def split(value):
    high = value.astype(BF16)
    return high, (value - high.astype(F32)).astype(BF16)


def mm(left, right):
    return jnp.dot(left, right, preferred_element_type=F32)


def wrap(index, count):
    return jnp.where(index < 0, index + count, index)


def grid_iota(rows, columns):
    return (
        lax.broadcasted_iota(jnp.int32, (rows, columns), 0),
        lax.broadcasted_iota(jnp.int32, (rows, columns), 1),
    )


def kernel(
    count_x, count_y,
    density_in, coupling_in, weights_in, live_in, pairs_in, dslot_in, fslot_in,
    out_ref,
    density_ref, coupling_ref, weights_ref, live_ref, pairs_ref, dslot_ref, fslot_ref,
    codes, refs_s, packed, held, note, held_note, chosen, got, joined,
    m_high, m_low, q_high, q_low, square,
    grown, landed, extra, landed_extra, flat, table, totals, back,
    send_sems, recv_sems, stage_sems,
):
    count = count_x * count_y
    dim_dev = coupling_ref.shape[0]
    refs = 2 * dim_dev
    dimers = dslot_ref.shape[0]
    width = density_ref.shape[1]
    half = width // 2
    near_y = count_y // 2
    team = count_x * near_y
    rows = width // team
    my_x, my_y = lax.axis_index("gx"), lax.axis_index("gy")
    me = my_x * count_y + my_y
    my_seat = my_x * near_y + lax.rem(my_y, near_y)
    first_y = my_y - lax.rem(my_y, near_y)
    spread_at, note_at, chosen_at = 0, 1, 2
    grown_at = chosen_at + 1
    extra_at = grown_at + refs
    total_at = extra_at + 1

    def peer(step):
        other = lax.rem(me + step, count)
        return other, (lax.div(other, count_y), lax.rem(other, count_y))

    def mate(step):
        seat = lax.rem(my_seat + step, team)
        x, y = lax.div(seat, near_y), first_y + lax.rem(seat, near_y)
        return x * count_y + y, (x, y)

    def seat_of(device):
        return lax.div(device, count_y) * near_y + lax.rem(lax.rem(device, count_y), near_y)

    barrier = pltpu.get_barrier_semaphore()

    def greet(step, carry):
        pl.semaphore_signal(barrier, inc=1, device_id=peer(step)[1], device_id_type=MESH)
        return carry

    lax.fori_loop(1, count, greet, 0)

    staged = [
        pltpu.make_async_copy(source, target, stage_sems.at[place])
        for place, (source, target) in enumerate((
            (density_in, density_ref), (dslot_in, dslot_ref), (fslot_in, fslot_ref),
            (pairs_in, pairs_ref), (weights_in, weights_ref), (live_in, live_ref),
            (coupling_in, coupling_ref),
        ))
    ]
    for copy in staged:
        copy.start()
    staged[0].wait()

    row_id, column_id = grid_iota(half, half)
    upper = row_id <= column_id
    strict = row_id > column_id
    on_diag = row_id == column_id

    def pack(first, corner, second):
        mixed = jnp.where(upper, first, second)
        return corner, mixed, jnp.sum(jnp.where(on_diag, second, 0.0), axis=0, keepdims=True)

    def scatter_rows(target, corner, mixed):
        for piece in range(team):
            start = piece * rows
            source = corner if start < half else mixed
            start = start % half
            target[piece] = source[start:start + rows]

    def factor_of(dimer):
        return jnp.where(live_ref[dimer] > 0, weights_ref[dimer], jnp.float32(0.0))

    corner, mixed, diag_row = pack(
        density_ref[0, :half, :half], density_ref[0, :half, half:], density_ref[0, half:, half:]
    )
    scatter_rows(packed, corner, mixed)
    for copy in staged[4:6]:
        copy.wait()
    note[0:1, :] = diag_row
    for dimer in range(dim_dev):
        note[dimer + 1:dimer + 2, :] = jnp.full((1, half), factor_of(dimer), F32)

    pl.semaphore_wait(barrier, count - 1)

    def push(phase, source, target, where_to):
        pltpu.make_async_remote_copy(
            src_ref=source,
            dst_ref=target,
            send_sem=send_sems.at[phase],
            recv_sem=recv_sems.at[phase],
            device_id=where_to,
            device_id_type=MESH,
        ).start()

    def visit(act, cycle):
        def at(turn, carry, lag):
            act(turn * cycle + lag)
            return carry

        for lag in sorted(range(cycle), key=lambda lag: -min(lag, cycle - lag)):
            lax.fori_loop(
                0 if lag else 1, count_x, functools.partial(at, lag=lag), 0, unroll=count_x <= 8
            )

    def to_all(phase, piece_for, target):
        def act(step):
            other, where_to = peer(step)
            push(phase, piece_for(other), target.at[count - step], where_to)

        visit(act, count_y)

    def to_team(phase, piece_for, target):
        def act(step):
            other, where_to = mate(step)
            push(phase, piece_for(other), target.at[team - step], where_to)

        visit(act, near_y)

    def drain(sems, phase, target, number):
        span = target.at[pl.ds(1, number - 1)]
        pltpu.make_async_copy(span, span, sems.at[phase]).wait()

    to_all(spread_at, lambda other: packed.at[seat_of(other)], held)
    to_all(note_at, lambda other: note, held_note)
    held[0] = packed[my_seat]
    held_note[0] = note[...]

    for copy in staged[1:4] + staged[6:]:
        copy.wait()

    def code_of(dimer, carry):
        codes[dimer] = fslot_ref[pairs_ref[0, dimer]] * count + fslot_ref[pairs_ref[1, dimer]]
        return carry

    lax.fori_loop(0, dimers, code_of, 0)

    def names(slot, carry):
        def look(dimer, found):
            return jnp.where(dslot_ref[dimer] == slot, codes[dimer], found)

        found = lax.fori_loop(0, dimers, look, jnp.int32(0), unroll=dimers <= 64)
        refs_s[2 * slot] = lax.div(found, jnp.int32(count))
        refs_s[2 * slot + 1] = lax.rem(found, jnp.int32(count))
        return carry

    lax.fori_loop(0, count * dim_dev, names, 0)

    drain(recv_sems, spread_at, held, count)

    def choose(seat, carry):
        target = lax.div(seat, near_y) * count_y + first_y + lax.rem(seat, near_y)
        for ref in range(refs):
            slot = refs_s[target * refs + ref]
            chosen[seat, ref] = held[wrap(slot - me, count)]
        return carry

    lax.fori_loop(0, team, choose, 0, unroll=team <= 32)
    to_team(chosen_at, lambda other: chosen.at[seat_of(other)], got)
    got[0] = chosen[my_seat]

    span = team * rows
    lanes = refs * span
    lane_id = lax.broadcasted_iota(jnp.int32, (1, lanes), 1)
    lane_entry = lane_id // rows

    def spread(entry, row):
        ref = lax.div(entry, team)
        source = mate(lax.rem(entry, team))[0]
        return jnp.where(lane_entry == entry, refs_s[source * refs + ref], row)

    named = lax.fori_loop(
        0, team * refs, spread, jnp.zeros((1, lanes), jnp.int32), unroll=team * refs <= 64
    )
    named = named * rows + lane_id % rows
    table_row = lax.broadcasted_iota(jnp.int32, (count * rows, lanes), 0)
    table[...] = jnp.where(table_row == named, 1.0, 0.0).astype(BF16)

    top, low = slice(0, width), slice(width, 2 * width)
    every = slice(0, 2 * width)

    def put(across, down, value):
        m_high[across, down], m_low[across, down] = split(value)

    def keep(across, down, value):
        square[across, down] = value
        q_high[across, down], q_low[across, down] = split(value)

    def times(left, across, middle, right, down):
        high, rest = left
        high_right, rest_right = right
        return (
            mm(high[across, middle], high_right[middle, down])
            + mm(high[across, middle], rest_right[middle, down])
            + mm(rest[across, middle], high_right[middle, down])
        )

    m_pair, q_pair = (m_high, m_low), (q_high, q_low)

    def couple(dimer):
        coupled = coupling_ref[dimer]
        put(top, low, coupled)
        put(low, top, coupled.T)
        square[top, top] = times(m_pair, top, low, m_pair, top)
        square[low, low] = times(m_pair, low, top, m_pair, low)

    def place(ref, side):
        for piece in range(team):
            joined[piece * rows:(piece + 1) * rows, :] = got[wrap(piece - my_seat, team), ref]
        corner = joined[:half, :]
        mixed = joined[half:, :]
        turned = mixed.T
        slot = refs_s[me * refs + ref]
        diag_row = held_note[wrap(slot - me, count), 0:1, :]
        start = side * width
        mid = start + half
        end = start + width
        put(slice(start, mid), slice(start, mid), jnp.where(upper, mixed, turned))
        put(slice(start, mid), slice(mid, end), corner)
        put(slice(mid, end), slice(start, mid), corner.T)
        put(
            slice(mid, end), slice(mid, end),
            jnp.where(on_diag, diag_row, jnp.where(strict, mixed, turned)),
        )

    def emit(ref, block):
        corner, mixed, diag_row = pack(block[:half, :half], block[:half, half:], block[half:, half:])
        scatter_rows(grown.at[ref], corner, mixed)
        extra[ref:ref + 1, :] = diag_row
        to_team(grown_at + ref, lambda other: grown.at[ref, seat_of(other)], landed.at[ref])

    couple(0)
    drain(recv_sems, note_at, held_note, count)
    drain(recv_sems, chosen_at, got, team)

    for dimer in range(dim_dev):
        first, second = 2 * dimer, 2 * dimer + 1
        factor = factor_of(dimer)
        if dimer:
            couple(dimer)
        place(first, 0)
        keep(top, top, square[top, top] + times(m_pair, top, top, m_pair, top))
        square[top, low] = times(m_pair, top, top, m_pair, low)
        place(second, 1)
        keep(top, low, square[top, low] + times(m_pair, top, low, m_pair, low))
        keep(low, low, square[low, low] + times(m_pair, low, low, m_pair, low))
        for repeat in range(ITERS - 1):
            across = 3.0 * square[top, low] - 2.0 * times(q_pair, top, every, m_pair, low)
            upper_left = 3.0 * square[top, top] - 2.0 * times(q_pair, top, every, m_pair, top)
            lower_right = 3.0 * square[low, low] - 2.0 * times(m_pair, low, every, q_pair, low)
            put(top, low, across)
            put(low, top, across.T)
            put(top, top, upper_left)
            put(low, low, lower_right)
            keep(top, top, times(m_pair, top, every, m_pair, top))
            keep(top, low, times(m_pair, top, every, m_pair, low))
            if repeat < ITERS - 2:
                keep(low, low, times(m_pair, low, every, m_pair, low))
        emit(first, factor * (
            3.0 * square[top, top] - 2.0 * times(q_pair, top, every, m_pair, top)
        ))
        keep(low, low, times(m_pair, low, every, m_pair, low))
        emit(second, factor * (
            3.0 * square[low, low] - 2.0 * times(m_pair, low, every, q_pair, low)
        ))

    to_all(extra_at, lambda other: extra, landed_extra)
    for ref in range(refs):
        landed[ref, 0] = grown[ref, my_seat]
    landed_extra[0] = extra[...]

    for ref in range(refs):
        drain(recv_sems, grown_at + ref, landed.at[ref], team)
        if rows % 8 == 0:
            values = landed[ref].reshape(span, half)
        else:
            for entry in range(team):
                flat[entry * rows:(entry + 1) * rows, :] = landed[ref, entry]
            values = flat[...]
        gained = mm(table[:, ref * span:(ref + 1) * span], jnp.concatenate(split(values), axis=1))
        gained = gained[:, :half] + gained[:, half:]
        sums = gained if ref == 0 else sums + gained
    for piece in range(count):
        totals[piece] = sums[piece * rows:(piece + 1) * rows, :]
    to_all(total_at, lambda other: totals.at[other], back)
    back[0] = totals[me]

    drain(recv_sems, extra_at, landed_extra, count)

    def collect(entry, carry):
        source = lax.rem(me + entry, count)
        diag_total, scale = carry
        for ref in range(refs):
            hit = jnp.where(refs_s[source * refs + ref] == me, 1, 0)
            mask = jnp.full((1, half), hit, jnp.int32) > 0
            diag_total = diag_total + jnp.where(mask, landed_extra[entry, ref:ref + 1, :], 0.0)
            row = 1 + ref // 2
            scale = scale + jnp.where(mask, held_note[entry, row:row + 1, :], 0.0)
        return diag_total, scale

    diag_total, scale = lax.fori_loop(
        0, count, collect, (jnp.zeros((1, half), F32), jnp.ones((1, half), F32)),
        unroll=count <= 32,
    )

    drain(recv_sems, total_at, back, count)
    for piece in range(team):
        source = piece // near_y * count_y + piece % near_y
        joined[piece * rows:(piece + 1) * rows, :] = (
            back[wrap(source - me, count)] + back[wrap(source + near_y - me, count)]
        )
    corner = joined[:half, :]
    mixed = joined[half:, :]
    turned = mixed.T
    out_ref[0, :half, :half] = (
        density_ref[0, :half, :half] + jnp.where(upper, mixed, turned)
    ) / scale
    out_ref[0, :half, half:] = (density_ref[0, :half, half:] + corner) / scale
    out_ref[0, half:, :half] = (density_ref[0, half:, :half] + corner.T) / scale
    out_ref[0, half:, half:] = (
        density_ref[0, half:, half:]
        + jnp.where(on_diag, diag_total, jnp.where(strict, mixed, turned))
    ) / scale

    drain(send_sems, spread_at, held, count)
    drain(send_sems, note_at, held_note, count)
    drain(send_sems, chosen_at, got, team)
    for ref in range(refs):
        drain(send_sems, grown_at + ref, landed.at[ref], team)
    drain(send_sems, extra_at, landed_extra, count)
    drain(send_sems, total_at, back, count)


def solution(mesh):
    count_x, count_y = mesh.shape["gx"], mesh.shape["gy"]
    count = count_x * count_y

    def per_device(density, coupling, weights, live_mask, dimer_pairs, dimer_slot, frag_slot):
        frag_dev, width, _ = density.shape
        dim_dev = coupling.shape[0]
        refs = 2 * dim_dev
        half = width // 2
        team = count // 2
        rows = width // team
        assert frag_dev == 1 and rows * team == width and count_y % 2 == 0
        vmem = lambda *shape: pltpu.VMEM(shape, F32)
        bf16 = lambda *shape: pltpu.VMEM(shape, BF16)
        in_vmem = pl.BlockSpec(memory_space=pltpu.VMEM)
        smem = lambda array: pltpu.SMEM(array.shape, array.dtype)
        pairs = dimer_pairs.T
        phases = 5 + refs
        return pl.pallas_call(
            functools.partial(kernel, count_x, count_y),
            out_shape=pltpu.VMEM(density.shape, F32),
            in_specs=[pl.BlockSpec(memory_space=pl.ANY)] * 7,
            out_specs=in_vmem,
            scratch_shapes=[
                vmem(*density.shape),
                vmem(*coupling.shape),
                smem(weights),
                smem(live_mask),
                smem(pairs),
                smem(dimer_slot),
                smem(frag_slot),
                pltpu.SMEM((dimer_slot.shape[0],), jnp.int32),
                pltpu.SMEM((count * refs,), jnp.int32),
                vmem(team, rows, half),
                vmem(count, rows, half),
                vmem(1 + dim_dev, half),
                vmem(count, 1 + dim_dev, half),
                vmem(team, refs, rows, half),
                vmem(team, refs, rows, half),
                vmem(width, half),
                bf16(2 * width, 2 * width),
                bf16(2 * width, 2 * width),
                bf16(2 * width, 2 * width),
                bf16(2 * width, 2 * width),
                vmem(2 * width, 2 * width),
                vmem(refs, team, rows, half),
                vmem(refs, team, rows, half),
                vmem(refs, half),
                vmem(count, refs, half),
                vmem(team * rows if rows % 8 else 8, half),
                bf16(count * rows, refs * team * rows),
                vmem(count, rows, half),
                vmem(count, rows, half),
                pltpu.SemaphoreType.DMA((phases,)),
                pltpu.SemaphoreType.DMA((phases,)),
                pltpu.SemaphoreType.DMA((7,)),
            ],
            compiler_params=pltpu.CompilerParams(collective_id=0, has_side_effects=True),
        )(density, coupling, weights, live_mask, pairs, dimer_slot, frag_slot)

    both = ("gx", "gy")
    return jax.shard_map(
        per_device,
        mesh=mesh,
        in_specs=(
            P(both, None, None),
            P(both, None, None),
            P(both),
            P(both),
            P(),
            P(),
            P(),
        ),
        out_specs=P(both, None, None),
        check_vma=False,
    )
```

```python
import functools
import jax
import jax.numpy as jnp
from jax import lax
from jax.experimental import pallas as pl
from jax.experimental.pallas import tpu as pltpu
from jax.sharding import PartitionSpec as P

ITERS = 3
MESH = pl.DeviceIdType.MESH
F32 = jnp.float32
BF16 = jnp.bfloat16


def split(value):
    high = value.astype(BF16)
    return high, (value - high.astype(F32)).astype(BF16)


def mm(left, right):
    return jnp.dot(left, right, preferred_element_type=F32)


def wrap(index, count):
    return jnp.where(index < 0, index + count, index)


def grid_iota(rows, columns):
    return (
        lax.broadcasted_iota(jnp.int32, (rows, columns), 0),
        lax.broadcasted_iota(jnp.int32, (rows, columns), 1),
    )


def kernel(
    count_x, count_y,
    density_in, coupling_in, weights_in, live_in, pairs_in, dslot_in, fslot_in,
    out_ref,
    density_ref, coupling_ref, weights_ref, live_ref, pairs_ref, dslot_ref, fslot_ref,
    codes, refs_s, packed, held, note, held_note, notice, mine, chosen, got, joined,
    m_high, m_low, q_high, q_low, square,
    grown_first, grown_second, landed_first, landed_second, flat, table, totals, back, cross, crossed,
    send_sems, recv_sems, stage_sems, ready,
):
    count = count_x * count_y
    dim_dev = coupling_ref.shape[0]
    refs = 2 * dim_dev
    dimers = dslot_ref.shape[0]
    width = density_ref.shape[1]
    half = width // 2
    near_y = count_y // 2
    team = count_x * near_y
    rows = width // team
    my_x, my_y = lax.axis_index("gx"), lax.axis_index("gy")
    me = my_x * count_y + my_y
    my_seat = my_x * near_y + lax.rem(my_y, near_y)
    first_y = my_y - lax.rem(my_y, near_y)
    far_y = lax.rem(my_y + near_y, count_y)
    spread_at, note_at, near_at, chosen_at, total_at, cross_at, grown_at = range(7)
    lane = lax.broadcasted_iota(jnp.int32, (1, half), 1)

    def peer(step):
        other = lax.rem(me + step, count)
        return other, (lax.div(other, count_y), lax.rem(other, count_y))

    def mate(step):
        seat = lax.rem(my_seat + step, team)
        x, y = lax.div(seat, near_y), first_y + lax.rem(seat, near_y)
        return x * count_y + y, (x, y)

    def seat_of(device):
        return lax.div(device, count_y) * near_y + lax.rem(lax.rem(device, count_y), near_y)

    staged = [
        pltpu.make_async_copy(source, target, stage_sems.at[place])
        for place, (source, target) in enumerate((
            (density_in, density_ref), (dslot_in, dslot_ref), (fslot_in, fslot_ref),
            (pairs_in, pairs_ref), (weights_in, weights_ref), (live_in, live_ref),
            (coupling_in, coupling_ref),
        ))
    ]
    for copy in staged:
        copy.start()

    barrier = pltpu.get_barrier_semaphore()
    quarter = count_y // 4
    early = my_y < near_y
    late = my_y >= count_y - quarter

    def planes(for_early, for_rest, act, between=None):
        def at(turn, carry, y):
            act(lax.rem(my_x + turn, count_x), y)
            return carry

        for place, (y_early, y_rest) in enumerate(zip(for_early, for_rest)):
            if between and place == len(for_early) - quarter:
                between()
            y = jnp.where(early, y_early, y_rest)
            pl.when(y != my_y)(functools.partial(act, my_x, y))
            lax.fori_loop(1, count_x, functools.partial(at, y=y), 0, unroll=count_x <= 8)

    near_first = (
        *range(near_y, count_y - quarter), *reversed(range(near_y)),
        *range(count_y - quarter, count_y),
    )
    across_first = tuple(range(count_y))

    def tell(semaphore, x, y):
        pl.semaphore_signal(semaphore, inc=1, device_id=(x, y), device_id_type=MESH)

    def greet(x, y):
        pl.when(jnp.logical_not(late & (y < near_y)))(
            functools.partial(tell, barrier, x, y)
        )

    planes(across_first, across_first, greet)
    staged[0].wait()

    row_id, column_id = grid_iota(half, half)
    upper = row_id <= column_id
    strict = row_id > column_id
    on_diag = row_id == column_id

    def pack(first, corner, second):
        mixed = jnp.where(upper, first, second)
        return corner, mixed, jnp.sum(jnp.where(on_diag, second, 0.0), axis=0, keepdims=True)

    def scatter_rows(target, corner, mixed):
        for piece in range(team):
            start = piece * rows
            source = corner if start < half else mixed
            start = start % half
            target[piece, :rows, :] = source[start:start + rows]

    def factor_of(dimer):
        return jnp.where(live_ref[dimer] > 0, weights_ref[dimer], jnp.float32(0.0))

    corner, mixed, diag_row = pack(
        density_ref[0, :half, :half], density_ref[0, :half, half:], density_ref[0, half:, half:]
    )
    scatter_rows(packed, corner, mixed)
    for copy in staged[4:6]:
        copy.wait()
    note[0:1, :] = diag_row
    for dimer in range(dim_dev):
        note[dimer + 1:dimer + 2, :] = jnp.where(lane == me, factor_of(dimer), jnp.float32(0.0))

    pl.when(early)(lambda: pl.semaphore_wait(barrier, count - quarter * count_x - 1))

    @pl.when(jnp.logical_not(early))
    def _():
        pl.semaphore_wait(barrier, count - 1)

        @pl.when(late)
        def _():
            for y in range(near_y):
                def at(turn, carry, y=y):
                    tell(ready, lax.rem(my_x + turn, count_x), y)
                    return carry

                lax.fori_loop(0, count_x, at, 0, unroll=count_x <= 8)

    def push(phase, source, target, where_to):
        pltpu.make_async_remote_copy(
            src_ref=source,
            dst_ref=target,
            send_sem=send_sems.at[phase],
            recv_sem=recv_sems.at[phase],
            device_id=where_to,
            device_id_type=MESH,
        ).start()

    def visit(act, cycle):
        def at(turn, carry, lag):
            act(turn * cycle + lag)
            return carry

        for lag in sorted(range(cycle), key=lambda lag: -min(lag, cycle - lag)):
            lax.fori_loop(
                0 if lag else 1, count_x, functools.partial(at, lag=lag), 0, unroll=count_x <= 8
            )

    def to_all(phase, piece_for, target):
        def act(step):
            other, where_to = peer(step)
            push(phase, piece_for(other), target.at[count - step], where_to)

        visit(act, count_y)

    def to_team(phase, piece_for, target):
        def act(step):
            other, where_to = mate(step)
            push(phase, piece_for(other), target.at[team - step], where_to)

        visit(act, near_y)

    def drain(sems, phase, target, number):
        span = target.at[pl.ds(1, number - 1)]
        pltpu.make_async_copy(span, span, sems.at[phase]).wait()

    def to_desks(act):
        for y in (0, near_y):
            pl.when((my_x != 0) | (my_y != y))(functools.partial(act, y))

    def deliver(x, y):
        other = x * count_y + y
        push(spread_at, packed.at[seat_of(other)], held.at[wrap(me - other, count)], (x, y))

    to_desks(lambda y: push(note_at, note, held_note.at[wrap(me - y, count)], (0, y)))
    planes(
        near_first, across_first, deliver,
        lambda: pl.when(early)(lambda: pl.semaphore_wait(ready, quarter * count_x)),
    )
    held[0] = packed[my_seat]

    for copy in staged[1:4] + staged[6:]:
        copy.wait()

    def code_of(dimer, carry):
        codes[dimer] = fslot_ref[pairs_ref[0, dimer]] * count + fslot_ref[pairs_ref[1, dimer]]
        return carry

    lax.fori_loop(0, dimers, code_of, 0)

    def names(slot, carry):
        def look(dimer, found):
            return jnp.where(dslot_ref[dimer] == slot, codes[dimer], found)

        found = lax.fori_loop(0, dimers, look, jnp.int32(0), unroll=dimers <= 64)
        refs_s[2 * slot] = lax.div(found, jnp.int32(count))
        refs_s[2 * slot + 1] = lax.rem(found, jnp.int32(count))
        return carry

    lax.fori_loop(0, count * dim_dev, names, 0)

    at_desk = my_seat == 0

    @pl.when(at_desk)
    def _():
        held_note[0] = note[...]
        drain(recv_sems, note_at, held_note, count)

        def gather(entry, rows):
            return rows + held_note[entry, 1:, :]

        factors = lax.fori_loop(
            0, count, gather, jnp.zeros((dim_dev, half), F32), unroll=count <= 32
        )

        def answer(seat, carry):
            target = lax.div(seat, near_y) * count_y + first_y + lax.rem(seat, near_y)
            for ref in range(refs):
                slot = refs_s[target * refs + ref]
                notice[seat, ref:ref + 1, :] = held_note[wrap(slot - me, count), 0:1, :]
            notice[seat, refs:, :] = factors
            return carry

        lax.fori_loop(0, team, answer, 0, unroll=team <= 32)

        def post(step):
            push(near_at, notice.at[step], mine, mate(step)[1])

        visit(post, near_y)
        mine[...] = notice[0]

    drain(recv_sems, spread_at, held, count)

    def choose(seat, carry):
        target = lax.div(seat, near_y) * count_y + first_y + lax.rem(seat, near_y)
        for ref in range(refs):
            slot = refs_s[target * refs + ref]
            chosen[seat, ref] = held[wrap(slot - me, count)]
        return carry

    lax.fori_loop(0, team, choose, 0, unroll=team <= 32)
    to_team(chosen_at, lambda other: chosen.at[seat_of(other)], got)
    got[0] = chosen[my_seat]

    span = team * rows
    lanes = refs * span
    lane_id = lax.broadcasted_iota(jnp.int32, (1, lanes), 1)
    lane_entry = lane_id // rows

    def spread(entry, row):
        ref = lax.div(entry, team)
        source = mate(lax.rem(entry, team))[0]
        return jnp.where(lane_entry == entry, refs_s[source * refs + ref], row)

    named = lax.fori_loop(
        0, team * refs, spread, jnp.zeros((1, lanes), jnp.int32), unroll=team * refs <= 64
    )
    named = named * rows + lane_id % rows
    table_row = lax.broadcasted_iota(jnp.int32, (count * rows, lanes), 0)
    table[...] = jnp.where(table_row == named, 1.0, 0.0).astype(BF16)

    top, low = slice(0, width), slice(width, 2 * width)
    every = slice(0, 2 * width)

    def put(across, down, value):
        m_high[across, down], m_low[across, down] = split(value)

    def keep(across, down, value):
        square[across, down] = value
        q_high[across, down], q_low[across, down] = split(value)

    def times(left, across, middle, right, down):
        high, rest = left
        high_right, rest_right = right
        return (
            mm(high[across, middle], high_right[middle, down])
            + mm(high[across, middle], rest_right[middle, down])
            + mm(rest[across, middle], high_right[middle, down])
        )

    m_pair, q_pair = (m_high, m_low), (q_high, q_low)

    def couple(dimer):
        coupled = coupling_ref[dimer]
        put(top, low, coupled)
        put(low, top, coupled.T)
        square[top, top] = times(m_pair, top, low, m_pair, top)
        square[low, low] = times(m_pair, low, top, m_pair, low)

    def place(ref, side):
        for piece in range(team):
            joined[piece * rows:(piece + 1) * rows, :] = got[wrap(piece - my_seat, team), ref]
        corner = joined[:half, :]
        mixed = joined[half:, :]
        turned = mixed.T
        diag_row = mine[ref:ref + 1, :]
        start = side * width
        mid = start + half
        end = start + width
        put(slice(start, mid), slice(start, mid), jnp.where(upper, mixed, turned))
        put(slice(start, mid), slice(mid, end), corner)
        put(slice(mid, end), slice(start, mid), corner.T)
        put(
            slice(mid, end), slice(mid, end),
            jnp.where(on_diag, diag_row, jnp.where(strict, mixed, turned)),
        )

    def grown(ref):
        return (grown_second if ref % 2 else grown_first).at[ref // 2]

    def landed(ref):
        return (landed_second if ref % 2 else landed_first).at[ref // 2]

    def emit(ref, block, other_row):
        corner, mixed, diag_row = pack(block[:half, :half], block[:half, half:], block[half:, half:])
        scatter_rows(grown(ref), corner, mixed)
        if ref % 2:
            for piece in range(team):
                grown(ref)[piece, rows:rows + 1, :] = other_row
                grown(ref)[piece, rows + 1:rows + 2, :] = diag_row
        to_team(grown_at + ref, lambda other: grown(ref).at[seat_of(other)], landed(ref))
        return diag_row

    couple(0)
    def count_hits(device, hits):
        for dimer in range(dim_dev):
            first = (device * dim_dev + dimer) * 2
            named_me = (refs_s[first] == me) | (refs_s[first + 1] == me)
            hit = jnp.where(named_me, 1.0, 0.0).astype(F32)
            hits = tuple(
                jnp.where(lane == device, hit, row) if place == dimer else row
                for place, row in enumerate(hits)
            )
        return hits

    hits = lax.fori_loop(
        0, count, count_hits, (jnp.zeros((1, half), F32),) * dim_dev, unroll=count <= 32
    )
    pl.when(jnp.logical_not(at_desk))(
        lambda: pltpu.make_async_copy(mine, mine, recv_sems.at[near_at]).wait()
    )
    scale = jnp.ones((1, 1), F32)
    for dimer in range(dim_dev):
        row = hits[dimer] * mine[refs + dimer:refs + dimer + 1, :]
        scale = scale + jnp.sum(row, axis=1, keepdims=True)
    drain(recv_sems, chosen_at, got, team)

    for dimer in range(dim_dev):
        first, second = 2 * dimer, 2 * dimer + 1
        factor = factor_of(dimer)
        if dimer:
            couple(dimer)
        place(first, 0)
        keep(top, top, square[top, top] + times(m_pair, top, top, m_pair, top))
        square[top, low] = times(m_pair, top, top, m_pair, low)
        place(second, 1)
        keep(top, low, square[top, low] + times(m_pair, top, low, m_pair, low))
        keep(low, low, square[low, low] + times(m_pair, low, low, m_pair, low))
        for repeat in range(ITERS - 1):
            across = 3.0 * square[top, low] - 2.0 * times(q_pair, top, every, m_pair, low)
            upper_left = 3.0 * square[top, top] - 2.0 * times(q_pair, top, every, m_pair, top)
            lower_right = 3.0 * square[low, low] - 2.0 * times(m_pair, low, every, q_pair, low)
            put(top, low, across)
            put(low, top, across.T)
            put(top, top, upper_left)
            put(low, low, lower_right)
            keep(top, top, times(m_pair, top, every, m_pair, top))
            keep(top, low, times(m_pair, top, every, m_pair, low))
            if repeat < ITERS - 2:
                keep(low, low, times(m_pair, low, every, m_pair, low))
        first_row = emit(first, factor * (
            3.0 * square[top, top] - 2.0 * times(q_pair, top, every, m_pair, top)
        ), None)
        keep(low, low, times(m_pair, low, every, m_pair, low))
        emit(second, factor * (
            3.0 * square[low, low] - 2.0 * times(m_pair, low, every, q_pair, low)
        ), first_row)

    for ref in range(refs):
        landed(ref)[0] = grown(ref)[my_seat]

    for ref in range(refs):
        drain(recv_sems, grown_at + ref, landed(ref), team)
        if rows % 8 == 0:
            values = landed(ref)[:, :rows, :].reshape(span, half)
        else:
            for entry in range(team):
                flat[entry * rows:(entry + 1) * rows, :] = landed(ref)[entry, :rows, :]
            values = flat[...]
        gained = mm(table[:, ref * span:(ref + 1) * span], jnp.concatenate(split(values), axis=1))
        gained = gained[:, :half] + gained[:, half:]
        sums = gained if ref == 0 else sums + gained
    for piece in range(count):
        totals[piece] = sums[piece * rows:(piece + 1) * rows, :]
    to_all(total_at, lambda other: totals.at[other], back)
    back[0] = totals[me]

    def collect(entry, sums):
        source = mate(entry)[0]
        for ref in range(refs):
            row = landed(ref | 1)[entry, rows + ref % 2:rows + ref % 2 + 1, :]
            named_at = refs_s[source * refs + ref]
            sums = tuple(
                total + jnp.where(jnp.full((1, half), named_at, jnp.int32) == owner, row, 0.0)
                for owner, total in zip((my_x * count_y + far_y, me), sums)
            )
        return sums

    cross_row, own_row = lax.fori_loop(
        0, team, collect, (jnp.zeros((1, half), F32),) * 2, unroll=team <= 32
    )
    cross[...] = cross_row
    push(cross_at, cross, crossed, (my_x, far_y))

    drain(recv_sems, total_at, back, count)
    for piece in range(team):
        source = piece // near_y * count_y + piece % near_y
        joined[piece * rows:(piece + 1) * rows, :] = (
            back[wrap(source - me, count)] + back[wrap(source + near_y - me, count)]
        )
    pltpu.make_async_copy(crossed, crossed, recv_sems.at[cross_at]).wait()
    diag_total = own_row + crossed[...]
    corner = joined[:half, :]
    mixed = joined[half:, :]
    turned = mixed.T
    out_ref[0, :half, :half] = (
        density_ref[0, :half, :half] + jnp.where(upper, mixed, turned)
    ) / scale
    out_ref[0, :half, half:] = (density_ref[0, :half, half:] + corner) / scale
    out_ref[0, half:, :half] = (density_ref[0, half:, :half] + corner.T) / scale
    out_ref[0, half:, half:] = (
        density_ref[0, half:, half:]
        + jnp.where(on_diag, diag_total, jnp.where(strict, mixed, turned))
    ) / scale

    drain(send_sems, spread_at, held, count)
    to_desks(lambda y: pltpu.make_async_copy(note, note, send_sems.at[note_at]).wait())
    pl.when(at_desk)(lambda: drain(send_sems, near_at, notice, team))
    drain(send_sems, chosen_at, got, team)
    for ref in range(refs):
        drain(send_sems, grown_at + ref, grown(ref), team)
    drain(send_sems, total_at, back, count)
    pltpu.make_async_copy(cross, cross, send_sems.at[cross_at]).wait()


def solution(mesh):
    count_x, count_y = mesh.shape["gx"], mesh.shape["gy"]
    count = count_x * count_y

    def per_device(density, coupling, weights, live_mask, dimer_pairs, dimer_slot, frag_slot):
        frag_dev, width, _ = density.shape
        dim_dev = coupling.shape[0]
        refs = 2 * dim_dev
        half = width // 2
        team = count // 2
        rows = width // team
        assert frag_dev == 1 and rows * team == width and count_y % 4 == 0 and count <= half
        vmem = lambda *shape: pltpu.VMEM(shape, F32)
        bf16 = lambda *shape: pltpu.VMEM(shape, BF16)
        in_vmem = pl.BlockSpec(memory_space=pltpu.VMEM)
        smem = lambda array: pltpu.SMEM(array.shape, array.dtype)
        pairs = dimer_pairs.T
        phases = 6 + refs
        return pl.pallas_call(
            functools.partial(kernel, count_x, count_y),
            out_shape=pltpu.VMEM(density.shape, F32),
            in_specs=[pl.BlockSpec(memory_space=pl.ANY)] * 7,
            out_specs=in_vmem,
            scratch_shapes=[
                vmem(*density.shape),
                vmem(*coupling.shape),
                smem(weights),
                smem(live_mask),
                smem(pairs),
                smem(dimer_slot),
                smem(frag_slot),
                pltpu.SMEM((dimer_slot.shape[0],), jnp.int32),
                pltpu.SMEM((count * refs,), jnp.int32),
                vmem(team, rows, half),
                vmem(count, rows, half),
                vmem(1 + dim_dev, half),
                vmem(count, 1 + dim_dev, half),
                vmem(team, refs + dim_dev, half),
                vmem(refs + dim_dev, half),
                vmem(team, refs, rows, half),
                vmem(team, refs, rows, half),
                vmem(width, half),
                bf16(2 * width, 2 * width),
                bf16(2 * width, 2 * width),
                bf16(2 * width, 2 * width),
                bf16(2 * width, 2 * width),
                vmem(2 * width, 2 * width),
                vmem(dim_dev, team, rows, half),
                vmem(dim_dev, team, rows + 2, half),
                vmem(dim_dev, team, rows, half),
                vmem(dim_dev, team, rows + 2, half),
                vmem(team * rows if rows % 8 else 8, half),
                bf16(count * rows, refs * team * rows),
                vmem(count, rows, half),
                vmem(count, rows, half),
                vmem(1, half),
                vmem(1, half),
                pltpu.SemaphoreType.DMA((phases,)),
                pltpu.SemaphoreType.DMA((phases,)),
                pltpu.SemaphoreType.DMA((7,)),
                pltpu.SemaphoreType.REGULAR,
            ],
            compiler_params=pltpu.CompilerParams(collective_id=0, has_side_effects=True),
        )(density, coupling, weights, live_mask, pairs, dimer_slot, frag_slot)

    both = ("gx", "gy")
    return jax.shard_map(
        per_device,
        mesh=mesh,
        in_specs=(
            P(both, None, None),
            P(both, None, None),
            P(both),
            P(both),
            P(),
            P(),
            P(),
        ),
        out_specs=P(both, None, None),
        check_vma=False,
    )
```

```python
import functools
import jax
import jax.numpy as jnp
from jax import lax
from jax.experimental import pallas as pl
from jax.experimental.pallas import tpu as pltpu
from jax.sharding import PartitionSpec as P

ITERS = 3
MESH = pl.DeviceIdType.MESH
F32 = jnp.float32
BF16 = jnp.bfloat16


def split(value):
    high = value.astype(BF16)
    return high, (value - high.astype(F32)).astype(BF16)


def mm(left, right):
    return jnp.dot(left, right, preferred_element_type=F32)


def wrap(index, count):
    return jnp.where(index < 0, index + count, index)


def grid_iota(rows, columns):
    return (
        lax.broadcasted_iota(jnp.int32, (rows, columns), 0),
        lax.broadcasted_iota(jnp.int32, (rows, columns), 1),
    )


def kernel(
    count_x, count_y,
    density_in, coupling_in, weights_in, live_in, pairs_in, dslot_in, fslot_in,
    out_ref,
    density_ref, coupling_ref, weights_ref, live_ref, pairs_ref, dslot_ref, fslot_ref,
    codes, refs_s, packed, held, note, held_note, notice, mine, chosen, got, joined,
    m_high, m_low, q_high, q_low, square,
    grown_first, grown_second, landed_first, landed_second, flat, table, totals, back, cross, crossed,
    send_sems, recv_sems, stage_sems, ready,
):
    count = count_x * count_y
    dim_dev = coupling_ref.shape[0]
    refs = 2 * dim_dev
    dimers = dslot_ref.shape[0]
    width = density_ref.shape[1]
    half = width // 2
    near_y = count_y // 2
    team = count_x * near_y
    rows = width // team
    my_x, my_y = lax.axis_index("gx"), lax.axis_index("gy")
    me = my_x * count_y + my_y
    my_seat = my_x * near_y + lax.rem(my_y, near_y)
    first_y = my_y - lax.rem(my_y, near_y)
    far_y = lax.rem(my_y + near_y, count_y)
    spread_at, note_at, near_at, chosen_at, total_at, cross_at, grown_at = range(7)
    lane = lax.broadcasted_iota(jnp.int32, (1, half), 1)

    def mate(step):
        seat = lax.rem(my_seat + step, team)
        x, y = lax.div(seat, near_y), first_y + lax.rem(seat, near_y)
        return x * count_y + y, (x, y)

    def seat_of(device):
        return lax.div(device, count_y) * near_y + lax.rem(lax.rem(device, count_y), near_y)

    staged = [
        pltpu.make_async_copy(source, target, stage_sems.at[place])
        for place, (source, target) in enumerate((
            (density_in, density_ref), (dslot_in, dslot_ref), (fslot_in, fslot_ref),
            (pairs_in, pairs_ref), (weights_in, weights_ref), (live_in, live_ref),
            (coupling_in, coupling_ref),
        ))
    ]
    for copy in staged:
        copy.start()

    barrier = pltpu.get_barrier_semaphore()
    quarter = count_y // 4
    early = my_y < near_y
    late = my_y >= count_y - quarter

    def column(turn):
        x, bit = my_x, 1
        while bit < count_x:
            toggle = bit - 2 * bit * lax.rem(lax.div(my_x, bit), 2)
            x = x + lax.rem(lax.div(count_x - 1 - turn, bit), 2) * toggle
            bit *= 2
        return x

    def plane(y, act):
        def at(turn, carry):
            act(column(turn), y)
            return carry

        lax.fori_loop(0, count_x - 1, at, 0, unroll=count_x <= 8)
        pl.when(y != my_y)(functools.partial(act, my_x, y))

    def planes(for_early, for_rest, act, between=None):
        for place, (y_early, y_rest) in enumerate(zip(for_early, for_rest)):
            if between and place == len(for_early) - quarter:
                between()
            plane(jnp.where(early, y_early, y_rest), act)

    near_first = (
        *range(near_y, count_y - quarter), *reversed(range(near_y)),
        *range(count_y - quarter, count_y),
    )
    across_first = tuple(range(count_y))
    far_first = sorted(range(count_y), key=lambda y: -abs(y - near_y + 1))
    far_first_rest = [count_y - 1 - y for y in far_first]

    def tell(semaphore, x, y):
        pl.semaphore_signal(semaphore, inc=1, device_id=(x, y), device_id_type=MESH)

    def greet(x, y):
        pl.when(jnp.logical_not(late) | (y >= count_y - quarter))(
            functools.partial(tell, barrier, x, y)
        )

    planes(across_first, across_first, greet)
    staged[0].wait()

    row_id, column_id = grid_iota(half, half)
    upper = row_id <= column_id
    strict = row_id > column_id
    on_diag = row_id == column_id

    def pack(first, corner, second):
        mixed = jnp.where(upper, first, second)
        return corner, mixed, jnp.sum(jnp.where(on_diag, second, 0.0), axis=0, keepdims=True)

    def scatter_rows(target, corner, mixed):
        for piece in range(team):
            start = piece * rows
            source = corner if start < half else mixed
            start = start % half
            target[piece, :rows, :] = source[start:start + rows]

    def factor_of(dimer):
        return jnp.where(live_ref[dimer] > 0, weights_ref[dimer], jnp.float32(0.0))

    corner, mixed, diag_row = pack(
        density_ref[0, :half, :half], density_ref[0, :half, half:], density_ref[0, half:, half:]
    )
    scatter_rows(packed, corner, mixed)
    for copy in staged[4:6]:
        copy.wait()
    note[0:1, :] = diag_row
    for dimer in range(dim_dev):
        note[dimer + 1:dimer + 2, :] = jnp.where(lane == me, factor_of(dimer), jnp.float32(0.0))

    pl.when(jnp.logical_not(late))(
        lambda: pl.semaphore_wait(barrier, count - quarter * count_x - 1)
    )

    @pl.when(late)
    def _():
        pl.semaphore_wait(barrier, count - 1)
        for y in range(count_y - quarter):
            plane(jnp.int32(y), functools.partial(tell, ready))

    def push(phase, source, target, where_to):
        pltpu.make_async_remote_copy(
            src_ref=source,
            dst_ref=target,
            send_sem=send_sems.at[phase],
            recv_sem=recv_sems.at[phase],
            device_id=where_to,
            device_id_type=MESH,
        ).start()

    def to_all(phase, piece_for, target):
        def act(x, y):
            other = x * count_y + y
            push(phase, piece_for(other), target.at[wrap(me - other, count)], (x, y))

        planes(far_first, far_first_rest, act)

    def team_planes(act):
        for lag in range(1, near_y + 1):
            plane(first_y + lax.rem(my_y - first_y + lag, near_y), act)

    def to_team(phase, piece_for, target):
        def act(x, y):
            seat = seat_of(x * count_y + y)
            push(phase, piece_for(seat), target.at[wrap(my_seat - seat, team)], (x, y))

        team_planes(act)

    def drain(sems, phase, target, number):
        span = target.at[pl.ds(1, number - 1)]
        pltpu.make_async_copy(span, span, sems.at[phase]).wait()

    def to_desks(act):
        for y in (0, near_y):
            pl.when((my_x != 0) | (my_y != y))(functools.partial(act, y))

    def deliver(x, y):
        other = x * count_y + y
        push(spread_at, packed.at[seat_of(other)], held.at[wrap(me - other, count)], (x, y))

    to_desks(lambda y: push(note_at, note, held_note.at[wrap(me - y, count)], (0, y)))
    planes(
        near_first, across_first, deliver,
        lambda: pl.when(jnp.logical_not(late))(
            lambda: pl.semaphore_wait(ready, quarter * count_x)
        ),
    )
    held[0] = packed[my_seat]

    for copy in staged[1:4] + staged[6:]:
        copy.wait()

    def code_of(dimer, carry):
        codes[dimer] = fslot_ref[pairs_ref[0, dimer]] * count + fslot_ref[pairs_ref[1, dimer]]
        return carry

    lax.fori_loop(0, dimers, code_of, 0)

    def names(slot, carry):
        def look(dimer, found):
            return jnp.where(dslot_ref[dimer] == slot, codes[dimer], found)

        found = lax.fori_loop(0, dimers, look, jnp.int32(0), unroll=dimers <= 64)
        refs_s[2 * slot] = lax.div(found, jnp.int32(count))
        refs_s[2 * slot + 1] = lax.rem(found, jnp.int32(count))
        return carry

    lax.fori_loop(0, count * dim_dev, names, 0)

    at_desk = my_seat == 0

    @pl.when(at_desk)
    def _():
        held_note[0] = note[...]
        drain(recv_sems, note_at, held_note, count)

        def gather(entry, rows):
            return rows + held_note[entry, 1:, :]

        factors = lax.fori_loop(
            0, count, gather, jnp.zeros((dim_dev, half), F32), unroll=count <= 32
        )

        def answer(seat, carry):
            target = lax.div(seat, near_y) * count_y + first_y + lax.rem(seat, near_y)
            for ref in range(refs):
                slot = refs_s[target * refs + ref]
                notice[seat, ref:ref + 1, :] = held_note[wrap(slot - me, count), 0:1, :]
            notice[seat, refs:, :] = factors
            return carry

        lax.fori_loop(0, team, answer, 0, unroll=team <= 32)

        def post(x, y):
            push(near_at, notice.at[seat_of(x * count_y + y)], mine, (x, y))

        team_planes(post)
        mine[...] = notice[0]

    drain(recv_sems, spread_at, held, count)

    def choose(seat, carry):
        target = lax.div(seat, near_y) * count_y + first_y + lax.rem(seat, near_y)
        for ref in range(refs):
            slot = refs_s[target * refs + ref]
            chosen[seat, ref] = held[wrap(slot - me, count)]
        return carry

    lax.fori_loop(0, team, choose, 0, unroll=team <= 32)
    to_team(chosen_at, lambda seat: chosen.at[seat], got)
    got[0] = chosen[my_seat]

    span = team * rows
    lanes = refs * span
    lane_id = lax.broadcasted_iota(jnp.int32, (1, lanes), 1)
    lane_entry = lane_id // rows

    def spread(entry, row):
        ref = lax.div(entry, team)
        source = mate(lax.rem(entry, team))[0]
        return jnp.where(lane_entry == entry, refs_s[source * refs + ref], row)

    named = lax.fori_loop(
        0, team * refs, spread, jnp.zeros((1, lanes), jnp.int32), unroll=team * refs <= 64
    )
    named = named * rows + lane_id % rows
    table_row = lax.broadcasted_iota(jnp.int32, (count * rows, lanes), 0)
    table[...] = jnp.where(table_row == named, 1.0, 0.0).astype(BF16)

    top, low = slice(0, width), slice(width, 2 * width)
    every = slice(0, 2 * width)

    def put(across, down, value):
        m_high[across, down], m_low[across, down] = split(value)

    def keep(across, down, value):
        square[across, down] = value
        q_high[across, down], q_low[across, down] = split(value)

    def times(left, across, middle, right, down):
        high, rest = left
        high_right, rest_right = right
        return (
            mm(high[across, middle], high_right[middle, down])
            + mm(high[across, middle], rest_right[middle, down])
            + mm(rest[across, middle], high_right[middle, down])
        )

    m_pair, q_pair = (m_high, m_low), (q_high, q_low)

    def couple(dimer):
        coupled = coupling_ref[dimer]
        put(top, low, coupled)
        put(low, top, coupled.T)
        square[top, top] = times(m_pair, top, low, m_pair, top)
        square[low, low] = times(m_pair, low, top, m_pair, low)

    def place(ref, side):
        for piece in range(team):
            joined[piece * rows:(piece + 1) * rows, :] = got[wrap(piece - my_seat, team), ref]
        corner = joined[:half, :]
        mixed = joined[half:, :]
        turned = mixed.T
        diag_row = mine[ref:ref + 1, :]
        start = side * width
        mid = start + half
        end = start + width
        put(slice(start, mid), slice(start, mid), jnp.where(upper, mixed, turned))
        put(slice(start, mid), slice(mid, end), corner)
        put(slice(mid, end), slice(start, mid), corner.T)
        put(
            slice(mid, end), slice(mid, end),
            jnp.where(on_diag, diag_row, jnp.where(strict, mixed, turned)),
        )

    def grown(ref):
        return (grown_second if ref % 2 else grown_first).at[ref // 2]

    def landed(ref):
        return (landed_second if ref % 2 else landed_first).at[ref // 2]

    def emit(ref, block, other_row):
        corner, mixed, diag_row = pack(block[:half, :half], block[:half, half:], block[half:, half:])
        scatter_rows(grown(ref), corner, mixed)
        if ref % 2:
            for piece in range(team):
                grown(ref)[piece, rows:rows + 1, :] = other_row
                grown(ref)[piece, rows + 1:rows + 2, :] = diag_row
        to_team(grown_at + ref, lambda seat: grown(ref).at[seat], landed(ref))
        return diag_row

    couple(0)
    def count_hits(device, hits):
        for dimer in range(dim_dev):
            first = (device * dim_dev + dimer) * 2
            named_me = (refs_s[first] == me) | (refs_s[first + 1] == me)
            hit = jnp.where(named_me, 1.0, 0.0).astype(F32)
            hits = tuple(
                jnp.where(lane == device, hit, row) if place == dimer else row
                for place, row in enumerate(hits)
            )
        return hits

    hits = lax.fori_loop(
        0, count, count_hits, (jnp.zeros((1, half), F32),) * dim_dev, unroll=count <= 32
    )
    pl.when(jnp.logical_not(at_desk))(
        lambda: pltpu.make_async_copy(mine, mine, recv_sems.at[near_at]).wait()
    )
    scale = jnp.ones((1, 1), F32)
    for dimer in range(dim_dev):
        row = hits[dimer] * mine[refs + dimer:refs + dimer + 1, :]
        scale = scale + jnp.sum(row, axis=1, keepdims=True)
    drain(recv_sems, chosen_at, got, team)

    for dimer in range(dim_dev):
        first, second = 2 * dimer, 2 * dimer + 1
        factor = factor_of(dimer)
        if dimer:
            couple(dimer)
        place(first, 0)
        keep(top, top, square[top, top] + times(m_pair, top, top, m_pair, top))
        square[top, low] = times(m_pair, top, top, m_pair, low)
        place(second, 1)
        keep(top, low, square[top, low] + times(m_pair, top, low, m_pair, low))
        keep(low, low, square[low, low] + times(m_pair, low, low, m_pair, low))
        for repeat in range(ITERS - 1):
            across = 3.0 * square[top, low] - 2.0 * times(q_pair, top, every, m_pair, low)
            upper_left = 3.0 * square[top, top] - 2.0 * times(q_pair, top, every, m_pair, top)
            lower_right = 3.0 * square[low, low] - 2.0 * times(m_pair, low, every, q_pair, low)
            put(top, low, across)
            put(low, top, across.T)
            put(top, top, upper_left)
            put(low, low, lower_right)
            keep(top, top, times(m_pair, top, every, m_pair, top))
            keep(top, low, times(m_pair, top, every, m_pair, low))
            if repeat < ITERS - 2:
                keep(low, low, times(m_pair, low, every, m_pair, low))
        first_row = emit(first, factor * (
            3.0 * square[top, top] - 2.0 * times(q_pair, top, every, m_pair, top)
        ), None)
        keep(low, low, times(m_pair, low, every, m_pair, low))
        emit(second, factor * (
            3.0 * square[low, low] - 2.0 * times(m_pair, low, every, q_pair, low)
        ), first_row)

    for ref in range(refs):
        landed(ref)[0] = grown(ref)[my_seat]

    for ref in range(refs):
        drain(recv_sems, grown_at + ref, landed(ref), team)
        if rows % 8 == 0:
            values = landed(ref)[:, :rows, :].reshape(span, half)
        else:
            for entry in range(team):
                flat[entry * rows:(entry + 1) * rows, :] = landed(ref)[entry, :rows, :]
            values = flat[...]
        gained = mm(table[:, ref * span:(ref + 1) * span], jnp.concatenate(split(values), axis=1))
        gained = gained[:, :half] + gained[:, half:]
        sums = gained if ref == 0 else sums + gained
    for piece in range(count):
        totals[piece] = sums[piece * rows:(piece + 1) * rows, :]
    to_all(total_at, lambda other: totals.at[other], back)
    back[0] = totals[me]

    def collect(entry, sums):
        source = mate(entry)[0]
        for ref in range(refs):
            row = landed(ref | 1)[entry, rows + ref % 2:rows + ref % 2 + 1, :]
            named_at = refs_s[source * refs + ref]
            sums = tuple(
                total + jnp.where(jnp.full((1, half), named_at, jnp.int32) == owner, row, 0.0)
                for owner, total in zip((my_x * count_y + far_y, me), sums)
            )
        return sums

    cross_row, own_row = lax.fori_loop(
        0, team, collect, (jnp.zeros((1, half), F32),) * 2, unroll=team <= 32
    )
    cross[...] = cross_row
    push(cross_at, cross, crossed, (my_x, far_y))

    drain(recv_sems, total_at, back, count)
    for piece in range(team):
        source = piece // near_y * count_y + piece % near_y
        joined[piece * rows:(piece + 1) * rows, :] = (
            back[wrap(source - me, count)] + back[wrap(source + near_y - me, count)]
        )
    pltpu.make_async_copy(crossed, crossed, recv_sems.at[cross_at]).wait()
    diag_total = own_row + crossed[...]
    corner = joined[:half, :]
    mixed = joined[half:, :]
    turned = mixed.T
    out_ref[0, :half, :half] = (
        density_ref[0, :half, :half] + jnp.where(upper, mixed, turned)
    ) / scale
    out_ref[0, :half, half:] = (density_ref[0, :half, half:] + corner) / scale
    out_ref[0, half:, :half] = (density_ref[0, half:, :half] + corner.T) / scale
    out_ref[0, half:, half:] = (
        density_ref[0, half:, half:]
        + jnp.where(on_diag, diag_total, jnp.where(strict, mixed, turned))
    ) / scale

    drain(send_sems, spread_at, held, count)
    to_desks(lambda y: pltpu.make_async_copy(note, note, send_sems.at[note_at]).wait())
    pl.when(at_desk)(lambda: drain(send_sems, near_at, notice, team))
    drain(send_sems, chosen_at, got, team)
    for ref in range(refs):
        drain(send_sems, grown_at + ref, grown(ref), team)
    drain(send_sems, total_at, back, count)
    pltpu.make_async_copy(cross, cross, send_sems.at[cross_at]).wait()


def solution(mesh):
    count_x, count_y = mesh.shape["gx"], mesh.shape["gy"]
    count = count_x * count_y

    def per_device(density, coupling, weights, live_mask, dimer_pairs, dimer_slot, frag_slot):
        frag_dev, width, _ = density.shape
        dim_dev = coupling.shape[0]
        refs = 2 * dim_dev
        half = width // 2
        team = count // 2
        rows = width // team
        assert frag_dev == 1 and rows * team == width and count_y % 4 == 0 and count <= half
        assert count_x & (count_x - 1) == 0
        vmem = lambda *shape: pltpu.VMEM(shape, F32)
        bf16 = lambda *shape: pltpu.VMEM(shape, BF16)
        in_vmem = pl.BlockSpec(memory_space=pltpu.VMEM)
        smem = lambda array: pltpu.SMEM(array.shape, array.dtype)
        pairs = dimer_pairs.T
        phases = 6 + refs
        return pl.pallas_call(
            functools.partial(kernel, count_x, count_y),
            out_shape=pltpu.VMEM(density.shape, F32),
            in_specs=[pl.BlockSpec(memory_space=pl.ANY)] * 7,
            out_specs=in_vmem,
            scratch_shapes=[
                vmem(*density.shape),
                vmem(*coupling.shape),
                smem(weights),
                smem(live_mask),
                smem(pairs),
                smem(dimer_slot),
                smem(frag_slot),
                pltpu.SMEM((dimer_slot.shape[0],), jnp.int32),
                pltpu.SMEM((count * refs,), jnp.int32),
                vmem(team, rows, half),
                vmem(count, rows, half),
                vmem(1 + dim_dev, half),
                vmem(count, 1 + dim_dev, half),
                vmem(team, refs + dim_dev, half),
                vmem(refs + dim_dev, half),
                vmem(team, refs, rows, half),
                vmem(team, refs, rows, half),
                vmem(width, half),
                bf16(2 * width, 2 * width),
                bf16(2 * width, 2 * width),
                bf16(2 * width, 2 * width),
                bf16(2 * width, 2 * width),
                vmem(2 * width, 2 * width),
                vmem(dim_dev, team, rows, half),
                vmem(dim_dev, team, rows + 2, half),
                vmem(dim_dev, team, rows, half),
                vmem(dim_dev, team, rows + 2, half),
                vmem(team * rows if rows % 8 else 8, half),
                bf16(count * rows, refs * team * rows),
                vmem(count, rows, half),
                vmem(count, rows, half),
                vmem(1, half),
                vmem(1, half),
                pltpu.SemaphoreType.DMA((phases,)),
                pltpu.SemaphoreType.DMA((phases,)),
                pltpu.SemaphoreType.DMA((7,)),
                pltpu.SemaphoreType.REGULAR,
            ],
            compiler_params=pltpu.CompilerParams(collective_id=0, has_side_effects=True),
        )(density, coupling, weights, live_mask, pairs, dimer_slot, frag_slot)

    both = ("gx", "gy")
    return jax.shard_map(
        per_device,
        mesh=mesh,
        in_specs=(
            P(both, None, None),
            P(both, None, None),
            P(both),
            P(both),
            P(),
            P(),
            P(),
        ),
        out_specs=P(both, None, None),
        check_vma=False,
    )
```

```python
import functools
import jax
import jax.numpy as jnp
from jax import lax
from jax.experimental import pallas as pl
from jax.experimental.pallas import tpu as pltpu
from jax.sharding import PartitionSpec as P

ITERS = 3
MESH = pl.DeviceIdType.MESH
F32 = jnp.float32
BF16 = jnp.bfloat16


def split(value):
    high = value.astype(BF16)
    return high, (value - high.astype(F32)).astype(BF16)


def mm(left, right):
    return jnp.dot(left, right, preferred_element_type=F32)


def wrap(index, count):
    return jnp.where(index < 0, index + count, index)


def grid_iota(rows, columns):
    return (
        lax.broadcasted_iota(jnp.int32, (rows, columns), 0),
        lax.broadcasted_iota(jnp.int32, (rows, columns), 1),
    )


def kernel(
    count_x, count_y,
    density_in, coupling_in, weights_in, live_in, pairs_in, dslot_in, fslot_in,
    out_ref,
    density_ref, coupling_ref, weights_ref, live_ref, pairs_ref, dslot_ref, fslot_ref,
    codes, refs_s, packed, held, note, held_note, notice, mine, chosen, got, joined,
    m_high, m_low, q_high, q_low, square,
    grown_first, grown_second, landed_first, landed_second, flat, table, totals, back, cross, crossed,
    send_sems, recv_sems, stage_sems, ready,
):
    count = count_x * count_y
    dim_dev = coupling_ref.shape[0]
    refs = 2 * dim_dev
    dimers = dslot_ref.shape[0]
    width = density_ref.shape[1]
    half = width // 2
    near_y = count_y // 2
    team = count_x * near_y
    rows = width // team
    my_x, my_y = lax.axis_index("gx"), lax.axis_index("gy")
    me = my_x * count_y + my_y
    my_seat = my_x * near_y + lax.rem(my_y, near_y)
    first_y = my_y - lax.rem(my_y, near_y)
    far_y = lax.rem(my_y + near_y, count_y)
    spread_at, note_at, near_at, chosen_at, total_at, cross_at, grown_at = range(7)
    lane = lax.broadcasted_iota(jnp.int32, (1, half), 1)

    def mate(step):
        seat = lax.rem(my_seat + step, team)
        x, y = lax.div(seat, near_y), first_y + lax.rem(seat, near_y)
        return x * count_y + y, (x, y)

    def seat_of(device):
        return lax.div(device, count_y) * near_y + lax.rem(lax.rem(device, count_y), near_y)

    staged = [
        pltpu.make_async_copy(source, target, stage_sems.at[place])
        for place, (source, target) in enumerate((
            (density_in, density_ref), (dslot_in, dslot_ref), (fslot_in, fslot_ref),
            (pairs_in, pairs_ref), (weights_in, weights_ref), (live_in, live_ref),
            (coupling_in, coupling_ref),
        ))
    ]
    for copy in staged:
        copy.start()

    barrier = pltpu.get_barrier_semaphore()
    quarter = count_y // 4
    early = my_y < near_y
    late = my_y >= count_y - quarter

    def column(turn):
        x, bit = my_x, 1
        while bit < count_x:
            toggle = bit - 2 * bit * lax.rem(lax.div(my_x, bit), 2)
            x = x + lax.rem(lax.div(count_x - 1 - turn, bit), 2) * toggle
            bit *= 2
        return x

    def plane(y, act):
        def at(turn, carry):
            act(column(turn), y)
            return carry

        lax.fori_loop(0, count_x - 1, at, 0, unroll=count_x <= 8)
        pl.when(y != my_y)(functools.partial(act, my_x, y))

    def planes(for_early, for_rest, act, between=None):
        for place, (y_early, y_rest) in enumerate(zip(for_early, for_rest)):
            if between and place == len(for_early) - quarter:
                between()
            plane(jnp.where(early, y_early, y_rest), act)

    near_first = (
        *range(near_y, count_y - quarter), *reversed(range(near_y)),
        *range(count_y - quarter, count_y),
    )
    across_first = tuple(range(count_y))
    def tell(semaphore, x, y):
        pl.semaphore_signal(semaphore, inc=1, device_id=(x, y), device_id_type=MESH)

    def greet(x, y):
        pl.when(jnp.logical_not(late) | (y >= count_y - quarter))(
            functools.partial(tell, barrier, x, y)
        )

    planes(across_first, across_first, greet)
    staged[0].wait()

    row_id, column_id = grid_iota(half, half)
    upper = row_id <= column_id
    strict = row_id > column_id
    on_diag = row_id == column_id

    def pack(first, corner, second):
        mixed = jnp.where(upper, first, second)
        return corner, mixed, jnp.sum(jnp.where(on_diag, second, 0.0), axis=0, keepdims=True)

    def scatter_rows(target, corner, mixed):
        for piece in range(team):
            start = piece * rows
            source = corner if start < half else mixed
            start = start % half
            target[piece, :rows, :] = source[start:start + rows]

    def factor_of(dimer):
        return jnp.where(live_ref[dimer] > 0, weights_ref[dimer], jnp.float32(0.0))

    corner, mixed, diag_row = pack(
        density_ref[0, :half, :half], density_ref[0, :half, half:], density_ref[0, half:, half:]
    )
    scatter_rows(packed, corner, mixed)
    for copy in staged[4:6]:
        copy.wait()
    note[0:1, :] = diag_row
    for dimer in range(dim_dev):
        note[dimer + 1:dimer + 2, :] = jnp.where(lane == me, factor_of(dimer), jnp.float32(0.0))

    pl.when(jnp.logical_not(late))(
        lambda: pl.semaphore_wait(barrier, count - quarter * count_x - 1)
    )

    @pl.when(late)
    def _():
        pl.semaphore_wait(barrier, count - 1)
        for y in range(count_y - quarter):
            plane(jnp.int32(y), functools.partial(tell, ready))

    def push(phase, source, target, where_to):
        pltpu.make_async_remote_copy(
            src_ref=source,
            dst_ref=target,
            send_sem=send_sems.at[phase],
            recv_sem=recv_sems.at[phase],
            device_id=where_to,
            device_id_type=MESH,
        ).start()

    def team_planes(act):
        for lag in range(1, near_y + 1):
            plane(first_y + lax.rem(my_y - first_y + lag, near_y), act)

    def to_team(phase, piece_for, target):
        def act(x, y):
            seat = seat_of(x * count_y + y)
            push(phase, piece_for(seat), target.at[wrap(my_seat - seat, team)], (x, y))

        team_planes(act)

    def drain(sems, phase, target, number):
        span = target.at[pl.ds(1, number - 1)]
        pltpu.make_async_copy(span, span, sems.at[phase]).wait()

    def to_desks(act):
        for y in (0, near_y):
            pl.when((my_x != 0) | (my_y != y))(functools.partial(act, y))

    def deliver(x, y):
        other = x * count_y + y
        push(spread_at, packed.at[seat_of(other)], held.at[wrap(me - other, count)], (x, y))

    to_desks(lambda y: push(note_at, note, held_note.at[wrap(me - y, count)], (0, y)))
    planes(
        near_first, across_first, deliver,
        lambda: pl.when(jnp.logical_not(late))(
            lambda: pl.semaphore_wait(ready, quarter * count_x)
        ),
    )
    held[0] = packed[my_seat]

    for copy in staged[1:4] + staged[6:]:
        copy.wait()

    def code_of(dimer, carry):
        codes[dimer] = fslot_ref[pairs_ref[0, dimer]] * count + fslot_ref[pairs_ref[1, dimer]]
        return carry

    lax.fori_loop(0, dimers, code_of, 0)

    def names(slot, carry):
        def look(dimer, found):
            return jnp.where(dslot_ref[dimer] == slot, codes[dimer], found)

        found = lax.fori_loop(0, dimers, look, jnp.int32(0), unroll=dimers <= 64)
        refs_s[2 * slot] = lax.div(found, jnp.int32(count))
        refs_s[2 * slot + 1] = lax.rem(found, jnp.int32(count))
        return carry

    lax.fori_loop(0, count * dim_dev, names, 0)

    at_desk = my_seat == 0

    @pl.when(at_desk)
    def _():
        held_note[0] = note[...]
        drain(recv_sems, note_at, held_note, count)

        def gather(entry, rows):
            return rows + held_note[entry, 1:, :]

        factors = lax.fori_loop(
            0, count, gather, jnp.zeros((dim_dev, half), F32), unroll=count <= 32
        )

        def answer(seat, carry):
            target = lax.div(seat, near_y) * count_y + first_y + lax.rem(seat, near_y)
            for ref in range(refs):
                slot = refs_s[target * refs + ref]
                notice[seat, ref:ref + 1, :] = held_note[wrap(slot - me, count), 0:1, :]
            notice[seat, refs:, :] = factors
            return carry

        lax.fori_loop(0, team, answer, 0, unroll=team <= 32)

        def post(x, y):
            push(near_at, notice.at[seat_of(x * count_y + y)], mine, (x, y))

        team_planes(post)
        mine[...] = notice[0]

    drain(recv_sems, spread_at, held, count)

    def choose(seat, carry):
        target = lax.div(seat, near_y) * count_y + first_y + lax.rem(seat, near_y)
        for ref in range(refs):
            slot = refs_s[target * refs + ref]
            chosen[seat, ref] = held[wrap(slot - me, count)]
        return carry

    lax.fori_loop(0, team, choose, 0, unroll=team <= 32)
    to_team(chosen_at, lambda seat: chosen.at[seat], got)
    got[0] = chosen[my_seat]

    span = team * rows
    lanes = refs * span
    lane_id = lax.broadcasted_iota(jnp.int32, (1, lanes), 1)
    lane_entry = lane_id // rows

    def owner_row(device):
        y = lax.rem(lax.rem(device, count_y) + count_y + near_y - first_y, count_y)
        return y * count_x + lax.div(device, count_y)

    def spread(entry, row):
        ref = lax.div(entry, team)
        source = mate(lax.rem(entry, team))[0]
        return jnp.where(lane_entry == entry, owner_row(refs_s[source * refs + ref]), row)

    named = lax.fori_loop(
        0, team * refs, spread, jnp.zeros((1, lanes), jnp.int32), unroll=team * refs <= 64
    )
    named = named * rows + lane_id % rows
    table_row = lax.broadcasted_iota(jnp.int32, (count * rows, lanes), 0)
    table[...] = jnp.where(table_row == named, 1.0, 0.0).astype(BF16)

    top, low = slice(0, width), slice(width, 2 * width)
    every = slice(0, 2 * width)

    def put(across, down, value):
        m_high[across, down], m_low[across, down] = split(value)

    def keep(across, down, value):
        square[across, down] = value
        q_high[across, down], q_low[across, down] = split(value)

    def times(left, across, middle, right, down):
        high, rest = left
        high_right, rest_right = right
        return (
            mm(high[across, middle], high_right[middle, down])
            + mm(high[across, middle], rest_right[middle, down])
            + mm(rest[across, middle], high_right[middle, down])
        )

    m_pair, q_pair = (m_high, m_low), (q_high, q_low)

    def couple(dimer):
        coupled = coupling_ref[dimer]
        put(top, low, coupled)
        put(low, top, coupled.T)
        square[top, top] = times(m_pair, top, low, m_pair, top)
        square[low, low] = times(m_pair, low, top, m_pair, low)

    def place(ref, side):
        for piece in range(team):
            joined[piece * rows:(piece + 1) * rows, :] = got[wrap(piece - my_seat, team), ref]
        corner = joined[:half, :]
        mixed = joined[half:, :]
        turned = mixed.T
        diag_row = mine[ref:ref + 1, :]
        start = side * width
        mid = start + half
        end = start + width
        put(slice(start, mid), slice(start, mid), jnp.where(upper, mixed, turned))
        put(slice(start, mid), slice(mid, end), corner)
        put(slice(mid, end), slice(start, mid), corner.T)
        put(
            slice(mid, end), slice(mid, end),
            jnp.where(on_diag, diag_row, jnp.where(strict, mixed, turned)),
        )

    def grown(ref):
        return (grown_second if ref % 2 else grown_first).at[ref // 2]

    def landed(ref):
        return (landed_second if ref % 2 else landed_first).at[ref // 2]

    def emit(ref, block, other_row):
        corner, mixed, diag_row = pack(block[:half, :half], block[:half, half:], block[half:, half:])
        scatter_rows(grown(ref), corner, mixed)
        if ref % 2:
            for piece in range(team):
                grown(ref)[piece, rows:rows + 1, :] = other_row
                grown(ref)[piece, rows + 1:rows + 2, :] = diag_row
        to_team(grown_at + ref, lambda seat: grown(ref).at[seat], landed(ref))
        return diag_row

    couple(0)
    def count_hits(device, hits):
        for dimer in range(dim_dev):
            first = (device * dim_dev + dimer) * 2
            named_me = (refs_s[first] == me) | (refs_s[first + 1] == me)
            hit = jnp.where(named_me, 1.0, 0.0).astype(F32)
            hits = tuple(
                jnp.where(lane == device, hit, row) if place == dimer else row
                for place, row in enumerate(hits)
            )
        return hits

    hits = lax.fori_loop(
        0, count, count_hits, (jnp.zeros((1, half), F32),) * dim_dev, unroll=count <= 32
    )
    pl.when(jnp.logical_not(at_desk))(
        lambda: pltpu.make_async_copy(mine, mine, recv_sems.at[near_at]).wait()
    )
    scale = jnp.ones((1, 1), F32)
    for dimer in range(dim_dev):
        row = hits[dimer] * mine[refs + dimer:refs + dimer + 1, :]
        scale = scale + jnp.sum(row, axis=1, keepdims=True)
    drain(recv_sems, chosen_at, got, team)

    for dimer in range(dim_dev):
        first, second = 2 * dimer, 2 * dimer + 1
        factor = factor_of(dimer)
        if dimer:
            couple(dimer)
        place(first, 0)
        keep(top, top, square[top, top] + times(m_pair, top, top, m_pair, top))
        square[top, low] = times(m_pair, top, top, m_pair, low)
        place(second, 1)
        keep(top, low, square[top, low] + times(m_pair, top, low, m_pair, low))
        keep(low, low, square[low, low] + times(m_pair, low, low, m_pair, low))
        for repeat in range(ITERS - 1):
            across = 3.0 * square[top, low] - 2.0 * times(q_pair, top, every, m_pair, low)
            upper_left = 3.0 * square[top, top] - 2.0 * times(q_pair, top, every, m_pair, top)
            lower_right = 3.0 * square[low, low] - 2.0 * times(m_pair, low, every, q_pair, low)
            put(top, low, across)
            put(low, top, across.T)
            put(top, top, upper_left)
            put(low, low, lower_right)
            keep(top, top, times(m_pair, top, every, m_pair, top))
            keep(top, low, times(m_pair, top, every, m_pair, low))
            if repeat < ITERS - 2:
                keep(low, low, times(m_pair, low, every, m_pair, low))
        keep(low, low, times(m_pair, low, every, m_pair, low))
        first_row = emit(first, factor * (
            3.0 * square[top, top] - 2.0 * times(q_pair, top, every, m_pair, top)
        ), None)
        emit(second, factor * (
            3.0 * square[low, low] - 2.0 * times(m_pair, low, every, q_pair, low)
        ), first_row)

    for ref in range(refs):
        landed(ref)[0] = grown(ref)[my_seat]

    def gain(ref, values, start, stop):
        block = table[start * rows:stop * rows, ref * span:(ref + 1) * span]
        gained = mm(block, values)
        return gained[:, :half] + gained[:, half:]

    sums = []
    for ref in range(refs):
        drain(recv_sems, grown_at + ref, landed(ref), team)
        if rows % 8 == 0:
            values = landed(ref)[:, :rows, :].reshape(span, half)
        else:
            for entry in range(team):
                flat[entry * rows:(entry + 1) * rows, :] = landed(ref)[entry, :rows, :]
            values = flat[...]
        values = jnp.concatenate(split(values), axis=1)
        if ref < refs - 1:
            added = [gain(ref, values, start, start + team) for start in (0, team)]
            sums = [a + b for a, b in zip(sums, added)] if sums else added

    def deal(side):
        start = side * team
        whole = sums[side] + gain(refs - 1, values, start, start + team)
        for piece in range(team):
            totals[start + piece] = whole[piece * rows:(piece + 1) * rows, :]

    def hand(x, y):
        other = x * count_y + y
        push(total_at, totals.at[owner_row(other)], back.at[wrap(me - other, count)], (x, y))

    deal(0)
    for lag in range(near_y):
        plane(jnp.where(early, count_y - 1 - lag, lag), hand)
    deal(1)
    team_planes(hand)
    back[0] = totals[owner_row(me)]

    def collect(entry, sums):
        source = mate(entry)[0]
        for ref in range(refs):
            row = landed(ref | 1)[entry, rows + ref % 2:rows + ref % 2 + 1, :]
            named_at = refs_s[source * refs + ref]
            sums = tuple(
                total + jnp.where(jnp.full((1, half), named_at, jnp.int32) == owner, row, 0.0)
                for owner, total in zip((my_x * count_y + far_y, me), sums)
            )
        return sums

    cross_row, own_row = lax.fori_loop(
        0, team, collect, (jnp.zeros((1, half), F32),) * 2, unroll=team <= 32
    )
    cross[...] = cross_row
    push(cross_at, cross, crossed, (my_x, far_y))

    drain(recv_sems, total_at, back, count)
    for piece in range(team):
        source = piece // near_y * count_y + piece % near_y
        joined[piece * rows:(piece + 1) * rows, :] = (
            back[wrap(source - me, count)] + back[wrap(source + near_y - me, count)]
        )
    pltpu.make_async_copy(crossed, crossed, recv_sems.at[cross_at]).wait()
    diag_total = own_row + crossed[...]
    corner = joined[:half, :]
    mixed = joined[half:, :]
    turned = mixed.T
    out_ref[0, :half, :half] = (
        density_ref[0, :half, :half] + jnp.where(upper, mixed, turned)
    ) / scale
    out_ref[0, :half, half:] = (density_ref[0, :half, half:] + corner) / scale
    out_ref[0, half:, :half] = (density_ref[0, half:, :half] + corner.T) / scale
    out_ref[0, half:, half:] = (
        density_ref[0, half:, half:]
        + jnp.where(on_diag, diag_total, jnp.where(strict, mixed, turned))
    ) / scale

    drain(send_sems, spread_at, held, count)
    to_desks(lambda y: pltpu.make_async_copy(note, note, send_sems.at[note_at]).wait())
    pl.when(at_desk)(lambda: drain(send_sems, near_at, notice, team))
    drain(send_sems, chosen_at, got, team)
    for ref in range(refs):
        drain(send_sems, grown_at + ref, grown(ref), team)
    drain(send_sems, total_at, back, count)
    pltpu.make_async_copy(cross, cross, send_sems.at[cross_at]).wait()


def solution(mesh):
    count_x, count_y = mesh.shape["gx"], mesh.shape["gy"]
    count = count_x * count_y

    def per_device(density, coupling, weights, live_mask, dimer_pairs, dimer_slot, frag_slot):
        frag_dev, width, _ = density.shape
        dim_dev = coupling.shape[0]
        refs = 2 * dim_dev
        half = width // 2
        team = count // 2
        rows = width // team
        assert frag_dev == 1 and rows * team == width and count_y % 4 == 0 and count <= half
        assert count_x & (count_x - 1) == 0
        vmem = lambda *shape: pltpu.VMEM(shape, F32)
        bf16 = lambda *shape: pltpu.VMEM(shape, BF16)
        in_vmem = pl.BlockSpec(memory_space=pltpu.VMEM)
        smem = lambda array: pltpu.SMEM(array.shape, array.dtype)
        pairs = dimer_pairs.T
        phases = 6 + refs
        return pl.pallas_call(
            functools.partial(kernel, count_x, count_y),
            out_shape=pltpu.VMEM(density.shape, F32),
            in_specs=[pl.BlockSpec(memory_space=pl.ANY)] * 7,
            out_specs=in_vmem,
            scratch_shapes=[
                vmem(*density.shape),
                vmem(*coupling.shape),
                smem(weights),
                smem(live_mask),
                smem(pairs),
                smem(dimer_slot),
                smem(frag_slot),
                pltpu.SMEM((dimer_slot.shape[0],), jnp.int32),
                pltpu.SMEM((count * refs,), jnp.int32),
                vmem(team, rows, half),
                vmem(count, rows, half),
                vmem(1 + dim_dev, half),
                vmem(count, 1 + dim_dev, half),
                vmem(team, refs + dim_dev, half),
                vmem(refs + dim_dev, half),
                vmem(team, refs, rows, half),
                vmem(team, refs, rows, half),
                vmem(width, half),
                bf16(2 * width, 2 * width),
                bf16(2 * width, 2 * width),
                bf16(2 * width, 2 * width),
                bf16(2 * width, 2 * width),
                vmem(2 * width, 2 * width),
                vmem(dim_dev, team, rows, half),
                vmem(dim_dev, team, rows + 2, half),
                vmem(dim_dev, team, rows, half),
                vmem(dim_dev, team, rows + 2, half),
                vmem(team * rows if rows % 8 else 8, half),
                bf16(count * rows, refs * team * rows),
                vmem(count, rows, half),
                vmem(count, rows, half),
                vmem(1, half),
                vmem(1, half),
                pltpu.SemaphoreType.DMA((phases,)),
                pltpu.SemaphoreType.DMA((phases,)),
                pltpu.SemaphoreType.DMA((7,)),
                pltpu.SemaphoreType.REGULAR,
            ],
            compiler_params=pltpu.CompilerParams(collective_id=0, has_side_effects=True),
        )(density, coupling, weights, live_mask, pairs, dimer_slot, frag_slot)

    both = ("gx", "gy")
    return jax.shard_map(
        per_device,
        mesh=mesh,
        in_specs=(
            P(both, None, None),
            P(both, None, None),
            P(both),
            P(both),
            P(),
            P(),
            P(),
        ),
        out_specs=P(both, None, None),
        check_vma=False,
    )
```

```python
import functools
import jax
import jax.numpy as jnp
from jax import lax
from jax.experimental import pallas as pl
from jax.experimental.pallas import tpu as pltpu
from jax.sharding import PartitionSpec as P

ITERS = 3
MESH = pl.DeviceIdType.MESH
F32 = jnp.float32
BF16 = jnp.bfloat16


def split(value):
    high = value.astype(BF16)
    return high, (value - high.astype(F32)).astype(BF16)


def mm(left, right):
    return jnp.dot(left, right, preferred_element_type=F32)


def wrap(index, count):
    return jnp.where(index < 0, index + count, index)


def grid_iota(rows, columns):
    return (
        lax.broadcasted_iota(jnp.int32, (rows, columns), 0),
        lax.broadcasted_iota(jnp.int32, (rows, columns), 1),
    )


def kernel(
    count_x, count_y,
    density_in, coupling_in, weights_in, live_in, pairs_in, dslot_in, fslot_in,
    out_ref,
    density_ref, coupling_ref, weights_ref, live_ref, pairs_ref, dslot_ref, fslot_ref,
    codes, refs_s, packed, held, note, held_note, notice, mine, chosen, got, joined,
    m_high, m_low, q_high, q_low, square,
    grown_first, grown_second, landed_first, landed_second, flat, table, totals, back, cross, crossed,
    send_sems, recv_sems, stage_sems, ready,
):
    count = count_x * count_y
    dim_dev = coupling_ref.shape[0]
    refs = 2 * dim_dev
    dimers = dslot_ref.shape[0]
    width = density_ref.shape[1]
    half = width // 2
    near_y = count_y // 2
    team = count_x * near_y
    rows = width // team
    my_x, my_y = lax.axis_index("gx"), lax.axis_index("gy")
    me = my_x * count_y + my_y
    my_seat = my_x * near_y + lax.rem(my_y, near_y)
    first_y = my_y - lax.rem(my_y, near_y)
    far_y = lax.rem(my_y + near_y, count_y)
    spread_at, note_at, near_at, chosen_at, total_at, cross_at, grown_at = range(7)
    lane = lax.broadcasted_iota(jnp.int32, (1, half), 1)

    def mate(step):
        seat = lax.rem(my_seat + step, team)
        x, y = lax.div(seat, near_y), first_y + lax.rem(seat, near_y)
        return x * count_y + y, (x, y)

    def seat_of(device):
        return lax.div(device, count_y) * near_y + lax.rem(lax.rem(device, count_y), near_y)

    staged = [
        pltpu.make_async_copy(source, target, stage_sems.at[place])
        for place, (source, target) in enumerate((
            (density_in, density_ref), (dslot_in, dslot_ref), (fslot_in, fslot_ref),
            (pairs_in, pairs_ref), (weights_in, weights_ref), (live_in, live_ref),
            (coupling_in, coupling_ref),
        ))
    ]
    for copy in staged:
        copy.start()

    barrier = pltpu.get_barrier_semaphore()
    quarter = count_y // 4
    early = my_y < near_y
    late = my_y >= count_y - quarter

    def column(turn):
        x, bit = my_x, 1
        while bit < count_x:
            toggle = bit - 2 * bit * lax.rem(lax.div(my_x, bit), 2)
            x = x + lax.rem(lax.div(count_x - 1 - turn, bit), 2) * toggle
            bit *= 2
        return x

    def plane(y, act):
        def at(turn, carry):
            act(column(turn), y)
            return carry

        lax.fori_loop(0, count_x - 1, at, 0, unroll=count_x <= 8)
        pl.when(y != my_y)(functools.partial(act, my_x, y))

    def planes(for_early, for_rest, act, between=None):
        for place, (y_early, y_rest) in enumerate(zip(for_early, for_rest)):
            if between and place == len(for_early) - quarter:
                between()
            plane(jnp.where(early, y_early, y_rest), act)

    near_first = (
        *range(near_y, count_y - quarter), *range(near_y),
        *range(count_y - quarter, count_y),
    )
    across_first = tuple(range(count_y))
    def tell(semaphore, x, y):
        pl.semaphore_signal(semaphore, inc=1, device_id=(x, y), device_id_type=MESH)

    def greet(x, y):
        pl.when(jnp.logical_not(late) | (y >= count_y - quarter))(
            functools.partial(tell, barrier, x, y)
        )

    planes(across_first, across_first, greet)
    staged[0].wait()

    row_id, column_id = grid_iota(half, half)
    upper = row_id <= column_id
    strict = row_id > column_id
    on_diag = row_id == column_id

    def pack(first, corner, second):
        mixed = jnp.where(upper, first, second)
        return corner, mixed, jnp.sum(jnp.where(on_diag, second, 0.0), axis=0, keepdims=True)

    def scatter_rows(target, corner, mixed):
        for piece in range(team):
            start = piece * rows
            source = corner if start < half else mixed
            start = start % half
            target[piece, :rows, :] = source[start:start + rows]

    def factor_of(dimer):
        return jnp.where(live_ref[dimer] > 0, weights_ref[dimer], jnp.float32(0.0))

    corner, mixed, diag_row = pack(
        density_ref[0, :half, :half], density_ref[0, :half, half:], density_ref[0, half:, half:]
    )
    scatter_rows(packed, corner, mixed)
    for copy in staged[4:6]:
        copy.wait()
    note[0:1, :] = diag_row
    for dimer in range(dim_dev):
        note[dimer + 1:dimer + 2, :] = jnp.where(lane == me, factor_of(dimer), jnp.float32(0.0))

    pl.when(jnp.logical_not(late))(
        lambda: pl.semaphore_wait(barrier, count - quarter * count_x - 1)
    )

    @pl.when(late)
    def _():
        pl.semaphore_wait(barrier, count - 1)
        for y in range(count_y - quarter):
            plane(jnp.int32(y), functools.partial(tell, ready))

    def push(phase, source, target, where_to):
        pltpu.make_async_remote_copy(
            src_ref=source,
            dst_ref=target,
            send_sem=send_sems.at[phase],
            recv_sem=recv_sems.at[phase],
            device_id=where_to,
            device_id_type=MESH,
        ).start()

    def team_planes(act):
        for lag in range(1, near_y + 1):
            plane(first_y + lax.rem(my_y - first_y + lag, near_y), act)

    def to_team(phase, piece_for, target):
        def act(x, y):
            seat = seat_of(x * count_y + y)
            push(phase, piece_for(seat), target.at[wrap(my_seat - seat, team)], (x, y))

        team_planes(act)

    def drain(sems, phase, target, number):
        span = target.at[pl.ds(1, number - 1)]
        pltpu.make_async_copy(span, span, sems.at[phase]).wait()

    def to_desks(act):
        for y in (0, near_y):
            pl.when((my_x != 0) | (my_y != y))(functools.partial(act, y))

    def deliver(x, y):
        other = x * count_y + y
        push(spread_at, packed.at[seat_of(other)], held.at[wrap(me - other, count)], (x, y))

    to_desks(lambda y: push(note_at, note, held_note.at[wrap(me - y, count)], (0, y)))
    planes(
        near_first, across_first, deliver,
        lambda: pl.when(jnp.logical_not(late))(
            lambda: pl.semaphore_wait(ready, quarter * count_x)
        ),
    )
    held[0] = packed[my_seat]

    for copy in staged[1:4] + staged[6:]:
        copy.wait()

    def code_of(dimer, carry):
        codes[dimer] = fslot_ref[pairs_ref[0, dimer]] * count + fslot_ref[pairs_ref[1, dimer]]
        return carry

    lax.fori_loop(0, dimers, code_of, 0)

    def names(slot, carry):
        def look(dimer, found):
            return jnp.where(dslot_ref[dimer] == slot, codes[dimer], found)

        found = lax.fori_loop(0, dimers, look, jnp.int32(0), unroll=dimers <= 64)
        refs_s[2 * slot] = lax.div(found, jnp.int32(count))
        refs_s[2 * slot + 1] = lax.rem(found, jnp.int32(count))
        return carry

    lax.fori_loop(0, count * dim_dev, names, 0)

    at_desk = my_seat == 0

    @pl.when(at_desk)
    def _():
        held_note[0] = note[...]
        drain(recv_sems, note_at, held_note, count)

        def gather(entry, rows):
            return rows + held_note[entry, 1:, :]

        factors = lax.fori_loop(
            0, count, gather, jnp.zeros((dim_dev, half), F32), unroll=count <= 32
        )

        def answer(seat, carry):
            target = lax.div(seat, near_y) * count_y + first_y + lax.rem(seat, near_y)
            for ref in range(refs):
                slot = refs_s[target * refs + ref]
                notice[seat, ref:ref + 1, :] = held_note[wrap(slot - me, count), 0:1, :]
            notice[seat, refs:, :] = factors
            return carry

        lax.fori_loop(0, team, answer, 0, unroll=team <= 32)

        def post(x, y):
            push(near_at, notice.at[seat_of(x * count_y + y)], mine, (x, y))

        team_planes(post)
        mine[...] = notice[0]

    drain(recv_sems, spread_at, held, count)

    def choose(seat, carry):
        target = lax.div(seat, near_y) * count_y + first_y + lax.rem(seat, near_y)
        for ref in range(refs):
            slot = refs_s[target * refs + ref]
            chosen[seat, ref] = held[wrap(slot - me, count)]
        return carry

    lax.fori_loop(0, team, choose, 0, unroll=team <= 32)
    to_team(chosen_at, lambda seat: chosen.at[seat], got)
    got[0] = chosen[my_seat]

    span = team * rows
    lanes = refs * span
    lane_id = lax.broadcasted_iota(jnp.int32, (1, lanes), 1)
    lane_entry = lane_id // rows

    def owner_row(device):
        y = lax.rem(lax.rem(device, count_y) + count_y + near_y - first_y, count_y)
        return y * count_x + lax.div(device, count_y)

    def spread(entry, row):
        ref = lax.div(entry, team)
        source = mate(lax.rem(entry, team))[0]
        return jnp.where(lane_entry == entry, owner_row(refs_s[source * refs + ref]), row)

    named = lax.fori_loop(
        0, team * refs, spread, jnp.zeros((1, lanes), jnp.int32), unroll=team * refs <= 64
    )
    named = named * rows + lane_id % rows
    table_row = lax.broadcasted_iota(jnp.int32, (count * rows, lanes), 0)
    table[...] = jnp.where(table_row == named, 1.0, 0.0).astype(BF16)

    top, low = slice(0, width), slice(width, 2 * width)
    every = slice(0, 2 * width)

    def put(across, down, value):
        m_high[across, down], m_low[across, down] = split(value)

    def keep(across, down, value):
        square[across, down] = value
        q_high[across, down], q_low[across, down] = split(value)

    def times(left, across, middle, right, down):
        high, rest = left
        high_right, rest_right = right
        return (
            mm(high[across, middle], high_right[middle, down])
            + mm(high[across, middle], rest_right[middle, down])
            + mm(rest[across, middle], high_right[middle, down])
        )

    m_pair, q_pair = (m_high, m_low), (q_high, q_low)

    def couple(dimer):
        coupled = coupling_ref[dimer]
        put(top, low, coupled)
        put(low, top, coupled.T)
        square[top, top] = times(m_pair, top, low, m_pair, top)
        square[low, low] = times(m_pair, low, top, m_pair, low)

    def place(ref, side):
        for piece in range(team):
            joined[piece * rows:(piece + 1) * rows, :] = got[wrap(piece - my_seat, team), ref]
        corner = joined[:half, :]
        mixed = joined[half:, :]
        turned = mixed.T
        diag_row = mine[ref:ref + 1, :]
        start = side * width
        mid = start + half
        end = start + width
        put(slice(start, mid), slice(start, mid), jnp.where(upper, mixed, turned))
        put(slice(start, mid), slice(mid, end), corner)
        put(slice(mid, end), slice(start, mid), corner.T)
        put(
            slice(mid, end), slice(mid, end),
            jnp.where(on_diag, diag_row, jnp.where(strict, mixed, turned)),
        )

    def grown(ref):
        return (grown_second if ref % 2 else grown_first).at[ref // 2]

    def landed(ref):
        return (landed_second if ref % 2 else landed_first).at[ref // 2]

    def emit(ref, block, other_row):
        corner, mixed, diag_row = pack(block[:half, :half], block[:half, half:], block[half:, half:])
        scatter_rows(grown(ref), corner, mixed)
        if ref % 2:
            for piece in range(team):
                grown(ref)[piece, rows:rows + 1, :] = other_row
                grown(ref)[piece, rows + 1:rows + 2, :] = diag_row
        to_team(grown_at + ref, lambda seat: grown(ref).at[seat], landed(ref))
        return diag_row

    couple(0)
    def count_hits(device, hits):
        for dimer in range(dim_dev):
            first = (device * dim_dev + dimer) * 2
            named_me = (refs_s[first] == me) | (refs_s[first + 1] == me)
            hit = jnp.where(named_me, 1.0, 0.0).astype(F32)
            hits = tuple(
                jnp.where(lane == device, hit, row) if place == dimer else row
                for place, row in enumerate(hits)
            )
        return hits

    hits = lax.fori_loop(
        0, count, count_hits, (jnp.zeros((1, half), F32),) * dim_dev, unroll=count <= 32
    )
    pl.when(jnp.logical_not(at_desk))(
        lambda: pltpu.make_async_copy(mine, mine, recv_sems.at[near_at]).wait()
    )
    scale = jnp.ones((1, 1), F32)
    for dimer in range(dim_dev):
        row = hits[dimer] * mine[refs + dimer:refs + dimer + 1, :]
        scale = scale + jnp.sum(row, axis=1, keepdims=True)
    drain(recv_sems, chosen_at, got, team)

    for dimer in range(dim_dev):
        first, second = 2 * dimer, 2 * dimer + 1
        factor = factor_of(dimer)
        if dimer:
            couple(dimer)
        place(first, 0)
        keep(top, top, square[top, top] + times(m_pair, top, top, m_pair, top))
        square[top, low] = times(m_pair, top, top, m_pair, low)
        place(second, 1)
        keep(top, low, square[top, low] + times(m_pair, top, low, m_pair, low))
        keep(low, low, square[low, low] + times(m_pair, low, low, m_pair, low))
        for repeat in range(ITERS - 1):
            across = 3.0 * square[top, low] - 2.0 * times(q_pair, top, every, m_pair, low)
            upper_left = 3.0 * square[top, top] - 2.0 * times(q_pair, top, every, m_pair, top)
            lower_right = 3.0 * square[low, low] - 2.0 * times(m_pair, low, every, q_pair, low)
            put(top, low, across)
            put(low, top, across.T)
            put(top, top, upper_left)
            put(low, low, lower_right)
            keep(top, top, times(m_pair, top, every, m_pair, top))
            keep(top, low, times(m_pair, top, every, m_pair, low))
            if repeat < ITERS - 2:
                keep(low, low, times(m_pair, low, every, m_pair, low))
        keep(low, low, times(m_pair, low, every, m_pair, low))
        first_row = emit(first, factor * (
            3.0 * square[top, top] - 2.0 * times(q_pair, top, every, m_pair, top)
        ), None)
        emit(second, factor * (
            3.0 * square[low, low] - 2.0 * times(m_pair, low, every, q_pair, low)
        ), first_row)

    for ref in range(refs):
        landed(ref)[0] = grown(ref)[my_seat]

    def gain(ref, values, start, stop):
        block = table[start * rows:stop * rows, ref * span:(ref + 1) * span]
        gained = mm(block, values)
        return gained[:, :half] + gained[:, half:]

    sums = []
    for ref in range(refs):
        drain(recv_sems, grown_at + ref, landed(ref), team)
        if rows % 8 == 0:
            values = landed(ref)[:, :rows, :].reshape(span, half)
        else:
            for entry in range(team):
                flat[entry * rows:(entry + 1) * rows, :] = landed(ref)[entry, :rows, :]
            values = flat[...]
        values = jnp.concatenate(split(values), axis=1)
        if ref < refs - 1:
            added = [gain(ref, values, start, start + team) for start in (0, team)]
            sums = [a + b for a, b in zip(sums, added)] if sums else added

    def deal(side):
        start = side * team
        whole = sums[side] + gain(refs - 1, values, start, start + team)
        for piece in range(team):
            totals[start + piece] = whole[piece * rows:(piece + 1) * rows, :]

    def hand(x, y):
        other = x * count_y + y
        push(total_at, totals.at[owner_row(other)], back.at[wrap(me - other, count)], (x, y))

    deal(0)
    for lag in range(near_y):
        plane(jnp.where(early, count_y - 1 - lag, lag), hand)
    deal(1)
    team_planes(hand)
    back[0] = totals[owner_row(me)]

    def collect(entry, sums):
        source = mate(entry)[0]
        for ref in range(refs):
            row = landed(ref | 1)[entry, rows + ref % 2:rows + ref % 2 + 1, :]
            named_at = refs_s[source * refs + ref]
            sums = tuple(
                total + jnp.where(jnp.full((1, half), named_at, jnp.int32) == owner, row, 0.0)
                for owner, total in zip((my_x * count_y + far_y, me), sums)
            )
        return sums

    cross_row, own_row = lax.fori_loop(
        0, team, collect, (jnp.zeros((1, half), F32),) * 2, unroll=team <= 32
    )
    cross[...] = cross_row
    push(cross_at, cross, crossed, (my_x, far_y))

    drain(recv_sems, total_at, back, count)
    for piece in range(team):
        source = piece // near_y * count_y + piece % near_y
        joined[piece * rows:(piece + 1) * rows, :] = (
            back[wrap(source - me, count)] + back[wrap(source + near_y - me, count)]
        )
    pltpu.make_async_copy(crossed, crossed, recv_sems.at[cross_at]).wait()
    diag_total = own_row + crossed[...]
    corner = joined[:half, :]
    mixed = joined[half:, :]
    turned = mixed.T
    out_ref[0, :half, :half] = (
        density_ref[0, :half, :half] + jnp.where(upper, mixed, turned)
    ) / scale
    out_ref[0, :half, half:] = (density_ref[0, :half, half:] + corner) / scale
    out_ref[0, half:, :half] = (density_ref[0, half:, :half] + corner.T) / scale
    out_ref[0, half:, half:] = (
        density_ref[0, half:, half:]
        + jnp.where(on_diag, diag_total, jnp.where(strict, mixed, turned))
    ) / scale

    drain(send_sems, spread_at, held, count)
    to_desks(lambda y: pltpu.make_async_copy(note, note, send_sems.at[note_at]).wait())
    pl.when(at_desk)(lambda: drain(send_sems, near_at, notice, team))
    drain(send_sems, chosen_at, got, team)
    for ref in range(refs):
        drain(send_sems, grown_at + ref, grown(ref), team)
    drain(send_sems, total_at, back, count)
    pltpu.make_async_copy(cross, cross, send_sems.at[cross_at]).wait()


def solution(mesh):
    count_x, count_y = mesh.shape["gx"], mesh.shape["gy"]
    count = count_x * count_y

    def per_device(density, coupling, weights, live_mask, dimer_pairs, dimer_slot, frag_slot):
        frag_dev, width, _ = density.shape
        dim_dev = coupling.shape[0]
        refs = 2 * dim_dev
        half = width // 2
        team = count // 2
        rows = width // team
        assert frag_dev == 1 and rows * team == width and count_y % 4 == 0 and count <= half
        assert count_x & (count_x - 1) == 0
        vmem = lambda *shape: pltpu.VMEM(shape, F32)
        bf16 = lambda *shape: pltpu.VMEM(shape, BF16)
        in_vmem = pl.BlockSpec(memory_space=pltpu.VMEM)
        smem = lambda array: pltpu.SMEM(array.shape, array.dtype)
        pairs = dimer_pairs.T
        phases = 6 + refs
        return pl.pallas_call(
            functools.partial(kernel, count_x, count_y),
            out_shape=pltpu.VMEM(density.shape, F32),
            in_specs=[pl.BlockSpec(memory_space=pl.ANY)] * 7,
            out_specs=in_vmem,
            scratch_shapes=[
                vmem(*density.shape),
                vmem(*coupling.shape),
                smem(weights),
                smem(live_mask),
                smem(pairs),
                smem(dimer_slot),
                smem(frag_slot),
                pltpu.SMEM((dimer_slot.shape[0],), jnp.int32),
                pltpu.SMEM((count * refs,), jnp.int32),
                vmem(team, rows, half),
                vmem(count, rows, half),
                vmem(1 + dim_dev, half),
                vmem(count, 1 + dim_dev, half),
                vmem(team, refs + dim_dev, half),
                vmem(refs + dim_dev, half),
                vmem(team, refs, rows, half),
                vmem(team, refs, rows, half),
                vmem(width, half),
                bf16(2 * width, 2 * width),
                bf16(2 * width, 2 * width),
                bf16(2 * width, 2 * width),
                bf16(2 * width, 2 * width),
                vmem(2 * width, 2 * width),
                vmem(dim_dev, team, rows, half),
                vmem(dim_dev, team, rows + 2, half),
                vmem(dim_dev, team, rows, half),
                vmem(dim_dev, team, rows + 2, half),
                vmem(team * rows if rows % 8 else 8, half),
                bf16(count * rows, refs * team * rows),
                vmem(count, rows, half),
                vmem(count, rows, half),
                vmem(1, half),
                vmem(1, half),
                pltpu.SemaphoreType.DMA((phases,)),
                pltpu.SemaphoreType.DMA((phases,)),
                pltpu.SemaphoreType.DMA((7,)),
                pltpu.SemaphoreType.REGULAR,
            ],
            compiler_params=pltpu.CompilerParams(collective_id=0, has_side_effects=True),
        )(density, coupling, weights, live_mask, pairs, dimer_slot, frag_slot)

    both = ("gx", "gy")
    return jax.shard_map(
        per_device,
        mesh=mesh,
        in_specs=(
            P(both, None, None),
            P(both, None, None),
            P(both),
            P(both),
            P(),
            P(),
            P(),
        ),
        out_specs=P(both, None, None),
        check_vma=False,
    )
```
